32 devices in a mesh: data: 1 (over z), expert: 32 (over y, x, core).
Axes of the slice: x: 4, y: 4, z: 1, core: 2. Of those that a mesh axis runs over, the one named last changes fastest.
The devices are a block of a 4x4x8 slice.
Arguments:
- x_a: bfloat16 [8192, 1024], P(('data', 'expert'))
- x_b: bfloat16 [8192, 1024], P(('data', 'expert'))
- dy_b: bfloat16 [8192, 1024], P(('data', 'expert'))
- eid_a: int32 [8192, 8], P(('data', 'expert'))
- slot_a: int32 [8192, 8], P(('data', 'expert'))
- gate_a: bfloat16 [8192, 8], P(('data', 'expert'))
- eid_b: int32 [8192, 8], P(('data', 'expert'))
- slot_b: int32 [8192, 8], P(('data', 'expert'))
- gate_b: bfloat16 [8192, 8], P(('data', 'expert'))
- u_b: bfloat16 [32, 4096, 1024], P(('data', 'expert'))
- norm_1: bfloat16 [1024], replicated
- norm_2: bfloat16 [1024], replicated
- w_q: bfloat16 [1024, 16, 64], replicated
- w_k: bfloat16 [1024, 8, 64], replicated
- w_v: bfloat16 [1024, 8, 64], replicated
- w_o: bfloat16 [16, 64, 1024], replicated
- w_1: bfloat16 [32, 1024, 512], P('expert')
- w_2: bfloat16 [32, 512, 1024], P('expert')
- w_3: bfloat16 [32, 1024, 512], P('expert')
Outputs:
- output 1: bfloat16 [8192, 1024], P(('data', 'expert'))
- output 2: bfloat16 [8192, 1024], P(('data', 'expert'))
- output 3: float32 [32, 1024, 512], P(('data', 'expert'))
- output 4: float32 [32, 512, 1024], P(('data', 'expert'))
- output 5: float32 [32, 1024, 512], P(('data', 'expert'))
- output 6: float32 [32, 1024, 16, 64], P(('data', 'expert'))
- output 7: float32 [32, 1024, 8, 64], P(('data', 'expert'))
- output 8: float32 [32, 1024, 8, 64], P(('data', 'expert'))
- output 9: float32 [32, 16, 64, 1024], P(('data', 'expert'))
- output 10: float32 [32, 1024], P(('data', 'expert'))
- output 11: float32 [32, 1024], P(('data', 'expert'))
All inputs are finite; a program needn't handle non-finite values.
Results may differ from the reference program's by a relative error of at most 0.0177277.
Values are sent between devices in bfloat16 or wider.
A program may use at most 768 MiB of HBM per device.

```python
import jax
import jax.numpy as jnp
from jax import lax

GROUP = 32
TOKENS = 256
MODEL_DIM = 1024
HEADS = 16
KV_HEADS = 8
HEAD_DIM = 64
EXPERTS = 32
FF_DIM = 512
TOP_K = 8
ROWS = GROUP * TOKENS
CAPACITY = ((2 * TOP_K * TOKENS + 8 * EXPERTS - 1) // (8 * EXPERTS)) * 8
HOT_ROWS = min(TOKENS, CAPACITY + CAPACITY // 4)
NORM_EPS = 1e-6


def draw_routing(route_key):
    key_score, key_hot = jax.random.split(route_key, 2)
    scores = jax.random.randint(key_score, (GROUP, TOKENS, EXPERTS), 0, 2 ** 20)
    hot_ids = jax.random.randint(key_hot, (GROUP,), 0, EXPERTS)
    boosted = (jnp.arange(TOKENS)[None, :, None] < HOT_ROWS) & (jnp.arange(EXPERTS)[None, None, :] == hot_ids[:, None, None])
    scores = (scores + boosted.astype(scores.dtype) * 2 ** 20) * EXPERTS + jnp.arange(EXPERTS)
    _, expert_ids = lax.top_k(scores, TOP_K)
    flat_ids = expert_ids.reshape(GROUP, TOKENS * TOP_K)
    onehot = (flat_ids[:, :, None] == jnp.arange(EXPERTS)[None, None, :]).astype(jnp.int32)
    arrival = jnp.sum((jnp.cumsum(onehot, axis=1) - onehot) * onehot, axis=2)
    slots = jnp.where(arrival < CAPACITY, arrival, -1)
    return expert_ids.reshape(ROWS, TOP_K).astype(jnp.int32), slots.reshape(ROWS, TOP_K).astype(jnp.int32)


def slot_columns(slots):
    device_of = jnp.arange(ROWS)[:, None] // TOKENS
    return jnp.where(slots >= 0, device_of * CAPACITY + slots, GROUP * CAPACITY)


def saved_inputs(value_key, expert_ids, slots):
    filled = jnp.zeros((EXPERTS, GROUP * CAPACITY), jnp.float32).at[expert_ids, slot_columns(slots)].set(1.0, mode='drop')
    values = jax.random.normal(value_key, (EXPERTS, GROUP * CAPACITY, MODEL_DIM), jnp.float32)
    return (values * filled[:, :, None]).astype(jnp.bfloat16)


def normal_draw(draw_key, dims, scale):
    return (jax.random.normal(draw_key, dims, jnp.float32) * scale).astype(jnp.bfloat16)


def setup_inputs(seed: int = 0, part: int = 0) -> dict:
    part_key = jax.random.fold_in(jax.random.key(seed), part)
    key_list = jax.random.split(part_key, 8)
    shared = jax.random.split(jax.random.key(seed + 1), 9)
    eid_a, slot_a = draw_routing(key_list[0])
    eid_b, slot_b = draw_routing(key_list[1])
    gate_a = (jax.random.uniform(key_list[2], (ROWS, TOP_K), jnp.float32, 0.5, 1.5) / TOP_K).astype(jnp.bfloat16)
    gate_b = (jax.random.uniform(key_list[3], (ROWS, TOP_K), jnp.float32, 0.5, 1.5) / TOP_K).astype(jnp.bfloat16)
    return {
        'x_a': normal_draw(key_list[4], (ROWS, MODEL_DIM), 1.0),
        'x_b': normal_draw(key_list[5], (ROWS, MODEL_DIM), 1.0),
        'dy_b': normal_draw(key_list[6], (ROWS, MODEL_DIM), 1.0),
        'eid_a': eid_a,
        'slot_a': slot_a,
        'gate_a': gate_a,
        'eid_b': eid_b,
        'slot_b': slot_b,
        'gate_b': gate_b,
        'u_b': saved_inputs(key_list[7], eid_b, slot_b),
        'norm_1': (1.0 + 0.3 * jax.random.normal(shared[0], (MODEL_DIM,), jnp.float32)).astype(jnp.bfloat16),
        'norm_2': (1.0 + 0.3 * jax.random.normal(shared[1], (MODEL_DIM,), jnp.float32)).astype(jnp.bfloat16),
        'w_q': normal_draw(shared[2], (MODEL_DIM, HEADS, HEAD_DIM), MODEL_DIM ** -0.5),
        'w_k': normal_draw(shared[3], (MODEL_DIM, KV_HEADS, HEAD_DIM), MODEL_DIM ** -0.5),
        'w_v': normal_draw(shared[4], (MODEL_DIM, KV_HEADS, HEAD_DIM), MODEL_DIM ** -0.5),
        'w_o': normal_draw(shared[5], (HEADS, HEAD_DIM, MODEL_DIM), 2.0 * (HEADS * HEAD_DIM) ** -0.5),
        'w_1': normal_draw(shared[6], (EXPERTS, MODEL_DIM, FF_DIM), MODEL_DIM ** -0.5),
        'w_2': normal_draw(shared[7], (EXPERTS, FF_DIM, MODEL_DIM), 3.0 * FF_DIM ** -0.5),
        'w_3': normal_draw(shared[8], (EXPERTS, MODEL_DIM, FF_DIM), MODEL_DIM ** -0.5),
    }


def rms_norm(values, gain):
    wide = values.astype(jnp.float32)
    scaled = wide * lax.rsqrt(jnp.mean(wide * wide, axis=-1, keepdims=True) + NORM_EPS)
    return (scaled * gain.astype(jnp.float32)).astype(jnp.bfloat16)


def add_rows(first, second):
    return (first.astype(jnp.float32) + second.astype(jnp.float32)).astype(jnp.bfloat16)


def attn_out(x_rows, norm_gain, w_q, w_k, w_v, w_o):
    normed = rms_norm(x_rows, norm_gain).astype(jnp.float32)
    query = jnp.einsum('td,dhe->the', normed, w_q.astype(jnp.float32)).astype(jnp.bfloat16)
    query = query.reshape(TOKENS, KV_HEADS, HEADS // KV_HEADS, HEAD_DIM).astype(jnp.float32)
    key_proj = jnp.einsum('td,dge->tge', normed, w_k.astype(jnp.float32)).astype(jnp.bfloat16).astype(jnp.float32)
    val_proj = jnp.einsum('td,dge->tge', normed, w_v.astype(jnp.float32)).astype(jnp.bfloat16).astype(jnp.float32)
    scores = jnp.einsum('tgre,mge->grtm', query, key_proj) * HEAD_DIM ** -0.5
    causal = jnp.arange(TOKENS)[:, None] >= jnp.arange(TOKENS)[None, :]
    scores = jnp.where(causal, scores, -1e30)
    probs = jax.nn.softmax(scores, axis=-1).astype(jnp.bfloat16).astype(jnp.float32)
    context = jnp.einsum('grtm,mge->tgre', probs, val_proj).astype(jnp.bfloat16)
    context = context.reshape(TOKENS, HEADS, HEAD_DIM).astype(jnp.float32)
    return jnp.einsum('the,hed->td', context, w_o.astype(jnp.float32)).astype(jnp.bfloat16)


def expert_forward(buf, w_1, w_2, w_3):
    act_1 = jnp.dot(buf, w_1, preferred_element_type=jnp.float32).astype(jnp.bfloat16).astype(jnp.float32)
    act_3 = jnp.dot(buf, w_3, preferred_element_type=jnp.float32).astype(jnp.bfloat16).astype(jnp.float32)
    hidden = (act_1 * jax.nn.sigmoid(act_1) * act_3).astype(jnp.bfloat16)
    return jnp.dot(hidden, w_2, preferred_element_type=jnp.float32).astype(jnp.bfloat16)


def expert_backward(saved, d_out, w_1, w_2, w_3):
    pre_1 = jnp.dot(saved, w_1, preferred_element_type=jnp.float32).astype(jnp.bfloat16).astype(jnp.float32)
    pre_3 = jnp.dot(saved, w_3, preferred_element_type=jnp.float32).astype(jnp.bfloat16).astype(jnp.float32)
    sigma = jax.nn.sigmoid(pre_1)
    silu_1 = pre_1 * sigma
    hidden = (silu_1 * pre_3).astype(jnp.bfloat16)
    grad_w2 = jnp.dot(hidden.T, d_out, preferred_element_type=jnp.float32)
    grad_hid = jnp.dot(d_out, w_2.T, preferred_element_type=jnp.float32).astype(jnp.bfloat16).astype(jnp.float32)
    grad_a1 = (grad_hid * pre_3 * sigma * (1.0 + pre_1 * (1.0 - sigma))).astype(jnp.bfloat16)
    grad_a3 = (grad_hid * silu_1).astype(jnp.bfloat16)
    grad_w1 = jnp.dot(saved.T, grad_a1, preferred_element_type=jnp.float32)
    grad_w3 = jnp.dot(saved.T, grad_a3, preferred_element_type=jnp.float32)
    grad_in = (jnp.dot(grad_a1, w_1.T, preferred_element_type=jnp.float32) + jnp.dot(grad_a3, w_3.T, preferred_element_type=jnp.float32)).astype(jnp.bfloat16)
    return grad_w1, grad_w2, grad_w3, grad_in


def pick_rows(buf, expert_ids, columns):
    padded = jnp.concatenate([buf, jnp.zeros((EXPERTS, 1, MODEL_DIM), buf.dtype)], axis=1)
    return padded[expert_ids, columns]


def reference(x_a, x_b, dy_b, eid_a, slot_a, gate_a, eid_b, slot_b, gate_b, u_b, norm_1, norm_2, w_q, w_k, w_v, w_o, w_1, w_2, w_3):
    def forward_rows(x_dev):
        return add_rows(x_dev, attn_out(x_dev, norm_1, w_q, w_k, w_v, w_o))
    h_a = lax.map(forward_rows, x_a.reshape(GROUP, TOKENS, MODEL_DIM)).reshape(ROWS, MODEL_DIM)
    u_a = rms_norm(h_a, norm_2)
    cols_a = slot_columns(slot_a)
    buf_a = jnp.zeros((EXPERTS, GROUP * CAPACITY, MODEL_DIM), jnp.bfloat16).at[eid_a, cols_a].set(jnp.broadcast_to(u_a[:, None, :], (ROWS, TOP_K, MODEL_DIM)), mode='drop')
    out_a = lax.map(lambda item: expert_forward(item[0], item[1], item[2], item[3]), (buf_a, w_1, w_2, w_3))
    picked = pick_rows(out_a, eid_a, cols_a).astype(jnp.float32)
    mixed = jnp.sum(gate_a.astype(jnp.float32)[:, :, None] * picked, axis=1)
    y_a = (h_a.astype(jnp.float32) + mixed).astype(jnp.bfloat16)
    cols_b = slot_columns(slot_b)
    grad_rows = (gate_b.astype(jnp.float32)[:, :, None] * dy_b.astype(jnp.float32)[:, None, :]).astype(jnp.bfloat16)
    d_out = jnp.zeros((EXPERTS, GROUP * CAPACITY, MODEL_DIM), jnp.bfloat16).at[eid_b, cols_b].set(grad_rows, mode='drop')
    grad_w1, grad_w2, grad_w3, grad_in = lax.map(lambda item: expert_backward(item[0], item[1], item[2], item[3], item[4]), (u_b, d_out, w_1, w_2, w_3))
    du_rows = jnp.sum(pick_rows(grad_in, eid_b, cols_b).astype(jnp.float32), axis=1).astype(jnp.bfloat16)
    def backward_rows(item):
        x_dev, dy_dev, du_dev = item
        attn_val, attn_pull = jax.vjp(attn_out, x_dev, norm_1, w_q, w_k, w_v, w_o)
        h_dev = add_rows(x_dev, attn_val)
        _, norm_pull = jax.vjp(rms_norm, h_dev, norm_2)
        dh_norm, grad_n2 = norm_pull(du_dev)
        dh_dev = add_rows(dy_dev, dh_norm)
        grad_x, grad_n1, grad_q, grad_k, grad_v, grad_o = attn_pull(dh_dev)
        return (add_rows(dh_dev, grad_x), grad_q.astype(jnp.float32), grad_k.astype(jnp.float32), grad_v.astype(jnp.float32), grad_o.astype(jnp.float32), grad_n1.astype(jnp.float32), grad_n2.astype(jnp.float32))
    dx_b, g_q, g_k, g_v, g_o, g_n1, g_n2 = lax.map(backward_rows, (x_b.reshape(GROUP, TOKENS, MODEL_DIM), dy_b.reshape(GROUP, TOKENS, MODEL_DIM), du_rows.reshape(GROUP, TOKENS, MODEL_DIM)))
    return (y_a, dx_b.reshape(ROWS, MODEL_DIM), grad_w1, grad_w2, grad_w3, g_q, g_k, g_v, g_o, g_n1, g_n2)
```

```python
import functools

import jax
import jax.numpy as jnp
from jax import lax
from jax.experimental import pallas as pl
from jax.experimental.pallas import tpu as pltpu
from jax.sharding import PartitionSpec as P

NORM_EPS = 1e-6
CORES = 2
BF16 = jnp.bfloat16
F32 = jnp.float32
MESH_ID = pl.DeviceIdType.MESH


def rms_norm(values, gain):
    wide = values.astype(jnp.float32)
    scaled = wide * lax.rsqrt(jnp.mean(wide * wide, axis=-1, keepdims=True) + NORM_EPS)
    return (scaled * gain.astype(jnp.float32)).astype(jnp.bfloat16)


def add_rows(first, second):
    return (first.astype(jnp.float32) + second.astype(jnp.float32)).astype(jnp.bfloat16)


def attn_out(x_rows, norm_gain, w_q, w_k, w_v, w_o):
    tokens = x_rows.shape[0]
    heads = w_q.shape[1]
    kv_heads = w_k.shape[1]
    head_dim = w_q.shape[2]
    normed = rms_norm(x_rows, norm_gain)
    query = jnp.einsum('td,dhe->the', normed, w_q, preferred_element_type=jnp.float32).astype(jnp.bfloat16)
    query = query.reshape(tokens, kv_heads, heads // kv_heads, head_dim)
    key_proj = jnp.einsum('td,dge->tge', normed, w_k, preferred_element_type=jnp.float32).astype(jnp.bfloat16)
    val_proj = jnp.einsum('td,dge->tge', normed, w_v, preferred_element_type=jnp.float32).astype(jnp.bfloat16)
    scores = jnp.einsum('tgre,mge->grtm', query, key_proj, preferred_element_type=jnp.float32) * head_dim ** -0.5
    causal = jnp.arange(tokens)[:, None] >= jnp.arange(tokens)[None, :]
    scores = jnp.where(causal, scores, -1e30)
    probs = jax.nn.softmax(scores, axis=-1).astype(jnp.bfloat16)
    context = jnp.einsum('grtm,mge->tgre', probs, val_proj, preferred_element_type=jnp.float32).astype(jnp.bfloat16)
    context = context.reshape(tokens, heads, head_dim)
    return jnp.einsum('the,hed->td', context, w_o, preferred_element_type=jnp.float32).astype(jnp.bfloat16)


def slot_tables(eid, slot, gate, experts):
    hit = eid[:, :, None] == jnp.arange(experts)[None, None, :]
    slots = jnp.sum(jnp.where(hit, slot[:, :, None] + 1, 0), axis=1) - 1
    gates = jnp.sum(jnp.where(hit, gate[:, :, None].astype(F32), 0.0), axis=1)
    return slots.astype(BF16), gates.astype(BF16)


def grid_of(group):
    side = int(round((group // CORES) ** 0.5))
    return side, group // CORES // side


def combine_kernel(side_y, side_x, o_ref, base_ref, meta_l, meta_r, out_ref, r1l, r1r, ps_l, ps_r, p2l, p2r, loc_sem, s1, v1, s2, v2):
    me = lax.axis_index('expert')
    core = me % CORES
    x = (me // CORES) % side_x
    y = me // (CORES * side_x)
    row_peers = side_x * CORES
    col_peers = side_y * CORES
    q_row = x * CORES + core
    q_col = y * CORES + core
    half = o_ref.shape[-1] // 2
    slots = o_ref.shape[-2]

    def dev(yy, xx, cc):
        return {'expert': (yy * side_x + xx) * CORES + cc}

    row_moves = [(dx, dc) for dx in range(side_x) for dc in range(CORES) if (dx, dc) != (0, 0)]
    col_moves = [(dy, dc) for dy in range(side_y) for dc in range(CORES) if (dy, dc) != (0, 0)]
    barrier = pltpu.get_barrier_semaphore()
    partners = [((y), (x + dx) % side_x, (core + dc) % CORES) for dx, dc in row_moves]
    partners += [((y + dy) % side_y, x, (core + dc) % CORES) for dy, dc in col_moves if dy]
    for spot in partners:
        pl.semaphore_signal(barrier, inc=1, device_id=dev(*spot), device_id_type=MESH_ID)
    pl.semaphore_wait(barrier, len(partners))

    def start_l(i, dx, dc):
        xt, ct = (x + dx) % side_x, (core + dc) % CORES
        copy = pltpu.make_async_remote_copy(src_ref=o_ref.at[:, xt, ct, :, pl.ds(0, half)], dst_ref=r1l.at[:, q_row], send_sem=s1.at[0, i], recv_sem=v1.at[0, i], device_id=dev(y, xt, ct), device_id_type=MESH_ID)
        copy.start()
        return copy

    def start_r(i, dy, dc):
        yt, ct = (y + dy) % side_y, (core + dc) % CORES
        copy = pltpu.make_async_remote_copy(src_ref=o_ref.at[yt, :, ct, :, pl.ds(half, half)], dst_ref=r1r.at[:, q_col], send_sem=s1.at[1, i], recv_sem=v1.at[1, i], device_id=dev(yt, x, ct), device_id_type=MESH_ID)
        copy.start()
        return copy

    first = []
    for i in range(max(len(row_moves), len(col_moves))):
        if i < len(row_moves):
            first.append(start_l(i, *row_moves[i]))
        if i < len(col_moves):
            first.append(start_r(i, *col_moves[i]))
    own_l = pltpu.make_async_copy(o_ref.at[:, x, core, :, pl.ds(0, half)], r1l.at[:, q_row], loc_sem.at[0])
    own_r = pltpu.make_async_copy(o_ref.at[y, :, core, :, pl.ds(half, half)], r1r.at[:, q_col], loc_sem.at[1])
    own_l.start()
    own_r.start()
    own_l.wait()
    own_r.wait()
    for copy in first:
        copy.wait()

    lane = lax.broadcasted_iota(jnp.int32, (1, slots), 1).astype(F32)

    def partial(meta, landed, sums, k, peers):
        table = meta[k].astype(F32)
        weights = []
        for q in range(peers):
            weights.append(jnp.where(table[:, q:q + 1] == lane, table[:, peers + q:peers + q + 1], 0.0).astype(BF16))
        weight = jnp.concatenate(weights, axis=1)
        vals = landed[k].reshape(peers * slots, half)
        sums[k] = jnp.dot(weight, vals, preferred_element_type=F32)

    def send_l(i):
        yt = (y + i) % side_y
        copy = pltpu.make_async_remote_copy(src_ref=ps_l.at[yt], dst_ref=p2l.at[i], send_sem=s2.at[0, i], recv_sem=v2.at[0, i], device_id=dev(yt, x, core), device_id_type=MESH_ID)
        copy.start()
        return copy

    def send_r(i):
        xt = (x + i) % side_x
        copy = pltpu.make_async_remote_copy(src_ref=ps_r.at[xt], dst_ref=p2r.at[i], send_sem=s2.at[1, i], recv_sem=v2.at[1, i], device_id=dev(y, xt, core), device_id_type=MESH_ID)
        copy.start()
        return copy

    second = []
    for i in range(1, max(side_y, side_x) + 1):
        if i < side_y:
            partial(meta_l, r1l, ps_l, (y + i) % side_y, row_peers)
        elif i == side_y:
            partial(meta_l, r1l, ps_l, y, row_peers)
        if 1 <= i - 1 < side_x:
            second.append(send_r(i - 1))
        if i < side_x:
            partial(meta_r, r1r, ps_r, (x + i) % side_x, col_peers)
        elif i == side_x:
            partial(meta_r, r1r, ps_r, x, col_peers)
        if i < side_y:
            second.append(send_l(i))
    for copy in second:
        copy.wait()
    total_l = base_ref[:, :half].astype(F32) + ps_l[y]
    for i in range(1, side_y):
        total_l = total_l + p2l[i]
    out_ref[:, :half] = total_l.astype(BF16)
    total_r = base_ref[:, half:].astype(F32) + ps_r[x]
    for i in range(1, side_x):
        total_r = total_r + p2r[i]
    out_ref[:, half:] = total_r.astype(BF16)


def combine(out_slots, base, meta_l, meta_r, group):
    side_y, side_x = grid_of(group)
    capacity = out_slots.shape[0] // group
    dim = out_slots.shape[-1]
    rows = base.shape[0]
    half = dim // 2
    cube = out_slots.reshape(side_y, side_x, CORES, capacity, dim)
    return pl.pallas_call(
        functools.partial(combine_kernel, side_y, side_x),
        out_shape=jax.ShapeDtypeStruct(base.shape, BF16),
        in_specs=[pl.BlockSpec(memory_space=pl.ANY)] + [pl.BlockSpec(memory_space=pltpu.VMEM)] * 3,
        out_specs=pl.BlockSpec(memory_space=pltpu.VMEM),
        scratch_shapes=[
            pltpu.VMEM((side_y, side_x * CORES, capacity, half), BF16),
            pltpu.VMEM((side_x, side_y * CORES, capacity, half), BF16),
            pltpu.VMEM((side_y, rows, half), F32),
            pltpu.VMEM((side_x, rows, half), F32),
            pltpu.VMEM((side_y, rows, half), F32),
            pltpu.VMEM((side_x, rows, half), F32),
            pltpu.SemaphoreType.DMA((2,)),
            pltpu.SemaphoreType.DMA((2, max(side_x, side_y) * CORES)),
            pltpu.SemaphoreType.DMA((2, max(side_x, side_y) * CORES)),
            pltpu.SemaphoreType.DMA((2, max(side_x, side_y))),
            pltpu.SemaphoreType.DMA((2, max(side_x, side_y))),
        ],
        compiler_params=pltpu.CompilerParams(collective_id=0, has_side_effects=True, vmem_limit_bytes=60000000),
    )(cube, base, meta_l, meta_r)


def combine_tables(slots, gates, group):
    side_y, side_x = grid_of(group)
    experts = slots.shape[-1]
    me = lax.axis_index('expert')
    core = me % CORES
    x = (me // CORES) % side_x
    y = me // (CORES * side_x)

    def cut(table):
        cube = table.reshape(side_y, side_x, CORES, -1, side_y, side_x, CORES)
        left = lax.dynamic_slice(cube, (0, x, core, 0, y, 0, 0), (side_y, 1, 1, cube.shape[3], 1, side_x, CORES))
        right = lax.dynamic_slice(cube, (y, 0, core, 0, 0, x, 0), (1, side_x, 1, cube.shape[3], side_y, 1, CORES))
        return left.reshape(side_y, -1, side_x * CORES), right.reshape(side_x, -1, side_y * CORES)
    sl, sr = cut(slots)
    gl, gr = cut(gates)
    return jnp.concatenate([sl, gl], axis=-1), jnp.concatenate([sr, gr], axis=-1)


def solution(mesh):
    group = mesh.shape['expert']

    def local_step(x_a, x_b, dy_b, eid_a, slot_a, gate_a, eid_b, slot_b, gate_b, u_b, norm_1, norm_2, w_q, w_k, w_v, w_o, w_1, w_2, w_3):
        experts = w_1.shape[0] * group
        capacity = u_b.shape[1] // group
        rows, model_dim = x_a.shape
        me = lax.axis_index('expert')
        w1, w2, w3 = w_1[0], w_2[0], w_3[0]

        tables = slot_tables(eid_a, slot_a, gate_a, experts) + slot_tables(eid_b, slot_b, gate_b, experts)
        meta = lax.all_gather(jnp.concatenate(tables, axis=1), 'expert', axis=0, tiled=True)
        dy_all = lax.all_gather(dy_b, 'expert', axis=0, tiled=True)
        slots_a, gates_a, slots_b, gates_b = [meta[:, i * experts:(i + 1) * experts] for i in range(4)]

        h_a = add_rows(x_a, attn_out(x_a, norm_1, w_q, w_k, w_v, w_o))
        u_a = rms_norm(h_a, norm_2)
        u_all = lax.all_gather(u_a, 'expert', axis=0, tiled=True)
        attn_val, attn_pull = jax.vjp(attn_out, x_b, norm_1, w_q, w_k, w_v, w_o)
        h_b = add_rows(x_b, attn_val)

        def mine(table):
            return lax.dynamic_slice_in_dim(table, me, 1, axis=1).reshape(group, 1, rows).astype(F32)

        place = jnp.arange(capacity, dtype=F32)[None, :, None]

        saved = u_b[0]
        pre_1 = jnp.dot(saved, w1, preferred_element_type=F32).astype(BF16).astype(F32)
        pre_3 = jnp.dot(saved, w3, preferred_element_type=F32).astype(BF16).astype(F32)
        sigma = jax.nn.sigmoid(pre_1)
        silu_1 = pre_1 * sigma
        hid_b = (silu_1 * pre_3).astype(BF16)
        pick_b = jnp.where(mine(slots_b) == place, mine(gates_b), 0.0).astype(BF16)
        d_out = jnp.einsum('pst,ptd->psd', pick_b, dy_all.reshape(group, rows, model_dim), preferred_element_type=F32).astype(BF16).reshape(group * capacity, model_dim)
        grad_hid = jnp.einsum('cd,fd->cf', d_out, w2, preferred_element_type=F32).astype(BF16).astype(F32)
        grad_a1 = (grad_hid * pre_3 * sigma * (1.0 + pre_1 * (1.0 - sigma))).astype(BF16)
        grad_a3 = (grad_hid * silu_1).astype(BF16)
        grad_in = (jnp.einsum('cf,df->cd', grad_a1, w1, preferred_element_type=F32) + jnp.einsum('cf,df->cd', grad_a3, w3, preferred_element_type=F32)).astype(BF16)
        ml, mr = combine_tables(slots_b, jnp.ones_like(gates_b), group)
        du = combine(grad_in, jnp.zeros_like(x_b), ml, mr, group)

        pick_a = (mine(slots_a) == place).astype(BF16)
        recv = jnp.einsum('pst,ptd->psd', pick_a, u_all.reshape(group, rows, model_dim), preferred_element_type=F32).astype(BF16).reshape(group * capacity, model_dim)
        act_1 = jnp.dot(recv, w1, preferred_element_type=F32).astype(BF16).astype(F32)
        act_3 = jnp.dot(recv, w3, preferred_element_type=F32).astype(BF16).astype(F32)
        hidden = (act_1 * jax.nn.sigmoid(act_1) * act_3).astype(BF16)
        out_a = jnp.dot(hidden, w2, preferred_element_type=F32).astype(BF16)
        ml, mr = combine_tables(slots_a, gates_a, group)
        y_a = combine(out_a, h_a, ml, mr, group)

        grad_w2 = jnp.einsum('cf,cd->fd', hid_b, d_out, preferred_element_type=F32)
        grad_w1 = jnp.einsum('cd,cf->df', saved, grad_a1, preferred_element_type=F32)
        grad_w3 = jnp.einsum('cd,cf->df', saved, grad_a3, preferred_element_type=F32)

        _, norm_pull = jax.vjp(rms_norm, h_b, norm_2)
        dh_norm, g_n2 = norm_pull(du)
        dh = add_rows(dy_b, dh_norm)
        grad_x, g_n1, g_q, g_k, g_v, g_o = attn_pull(dh)
        dx_b = add_rows(dh, grad_x)
        grads = [g.astype(F32)[None] for g in (g_q, g_k, g_v, g_o, g_n1, g_n2)]
        return (y_a, dx_b, grad_w1[None], grad_w2[None], grad_w3[None], *grads)

    row_spec = P(('data', 'expert'), None)
    cube_spec = P(('data', 'expert'), None, None)
    quad_spec = P(('data', 'expert'), None, None, None)
    expert_spec = P('expert', None, None)
    in_specs = (row_spec, row_spec, row_spec, row_spec, row_spec, row_spec, row_spec, row_spec, row_spec, cube_spec, P(), P(), P(), P(), P(), P(), expert_spec, expert_spec, expert_spec)
    out_specs = (row_spec, row_spec, cube_spec, cube_spec, cube_spec, quad_spec, quad_spec, quad_spec, quad_spec, row_spec, row_spec)
    return jax.shard_map(local_step, mesh=mesh, in_specs=in_specs, out_specs=out_specs, check_vma=False)
```

```python
import functools

import jax
import jax.numpy as jnp
from jax import lax
from jax.experimental import pallas as pl
from jax.experimental.pallas import tpu as pltpu
from jax.sharding import PartitionSpec as P

NORM_EPS = 1e-6
CORES = 2
BF16 = jnp.bfloat16
F32 = jnp.float32
MESH_ID = pl.DeviceIdType.MESH


def rms_norm(values, gain):
    wide = values.astype(jnp.float32)
    scaled = wide * lax.rsqrt(jnp.mean(wide * wide, axis=-1, keepdims=True) + NORM_EPS)
    return (scaled * gain.astype(jnp.float32)).astype(jnp.bfloat16)


def add_rows(first, second):
    return (first.astype(jnp.float32) + second.astype(jnp.float32)).astype(jnp.bfloat16)


def attn_out(x_rows, norm_gain, w_q, w_k, w_v, w_o):
    tokens = x_rows.shape[0]
    heads = w_q.shape[1]
    kv_heads = w_k.shape[1]
    head_dim = w_q.shape[2]
    normed = rms_norm(x_rows, norm_gain)
    query = jnp.einsum('td,dhe->the', normed, w_q, preferred_element_type=jnp.float32).astype(jnp.bfloat16)
    query = query.reshape(tokens, kv_heads, heads // kv_heads, head_dim)
    key_proj = jnp.einsum('td,dge->tge', normed, w_k, preferred_element_type=jnp.float32).astype(jnp.bfloat16)
    val_proj = jnp.einsum('td,dge->tge', normed, w_v, preferred_element_type=jnp.float32).astype(jnp.bfloat16)
    scores = jnp.einsum('tgre,mge->grtm', query, key_proj, preferred_element_type=jnp.float32) * head_dim ** -0.5
    causal = jnp.arange(tokens)[:, None] >= jnp.arange(tokens)[None, :]
    scores = jnp.where(causal, scores, -1e30)
    probs = jax.nn.softmax(scores, axis=-1).astype(jnp.bfloat16)
    context = jnp.einsum('grtm,mge->tgre', probs, val_proj, preferred_element_type=jnp.float32).astype(jnp.bfloat16)
    context = context.reshape(tokens, heads, head_dim)
    return jnp.einsum('the,hed->td', context, w_o, preferred_element_type=jnp.float32).astype(jnp.bfloat16)


def slot_tables(eid, slot, gate, experts):
    hit = eid[:, :, None] == jnp.arange(experts)[None, None, :]
    slots = jnp.sum(jnp.where(hit, slot[:, :, None] + 1, 0), axis=1) - 1
    gates = jnp.sum(jnp.where(hit, gate[:, :, None].astype(F32), 0.0), axis=1)
    return slots.astype(BF16), gates.astype(BF16)


def place_of(side_x):
    me = lax.axis_index('expert')
    core = me % CORES
    return me, me // (CORES * side_x), (me // CORES) % side_x, core


def dev(side_x, yy, xx, cc):
    return {'expert': (yy * side_x + xx) * CORES + cc}


def greet(partners):
    barrier = pltpu.get_barrier_semaphore()
    for spot in partners:
        pl.semaphore_signal(barrier, inc=1, device_id=spot, device_id_type=MESH_ID)
    pl.semaphore_wait(barrier, len(partners))


class Gather:
    def __init__(self, side, buf, cut, send, recv):
        self.side, self.buf, self.send, self.recv = side, buf, send, recv
        _, self.y, self.x, self.core = place_of(side)
        width = buf.shape[-1]
        self.left, self.right = pl.ds(0, cut), pl.ds(cut, width - cut)
        self.count = 0
        y, x, c, side = self.y, self.x, self.core, self.side
        up, down, far = (y + 1) % side, (y + side - 1) % side, (y + 2) % side
        east, west, over = (x + 1) % side, (x + side - 1) % side, (x + 2) % side
        pair = side // 2
        lo, hi, every = pl.ds(0, pair), pl.ds(pair, pair), pl.ds(0, side)
        twin = 1 - c
        L, R = self.left, self.right
        self.own = []
        for k in (1, side - 1, 2):
            self.own.append(self.make((y, x, c, L), (y, (x + k) % side, c)))
            self.own.append(self.make((y, x, c, R), ((y + k) % side, x, c)))
        self.line = [self.make((y, every, c, L), (up, x, c)), self.make((every, x, c, R), (y, east, c)),
                     self.make((y, every, c, L), (down, x, c)), self.make((every, x, c, R), (y, west, c))]
        self.relay = [self.make((down, lo, c, L), (up, x, c)), self.make((lo, west, c, R), (y, east, c)),
                      self.make((up, hi, c, L), (down, x, c)), self.make((hi, east, c, R), (y, west, c))]
        self.twin_own = [self.make((y, every, c, L), (y, x, twin)), self.make((every, x, c, R), (y, x, twin))]
        self.twin_line = [self.make((up, every, c, L), (y, x, twin)), self.make((every, east, c, R), (y, x, twin)),
                          self.make((down, every, c, L), (y, x, twin)), self.make((every, west, c, R), (y, x, twin))]
        self.twin_far = [self.make((far, every, c, L), (y, x, twin)), self.make((every, over, c, R), (y, x, twin))]

    def make(self, spot, target):
        yy, xx, cc, cols = spot
        part = self.buf.at[yy, xx, cc, :, cols]
        i = self.count
        self.count += 1
        return pltpu.make_async_remote_copy(src_ref=part, dst_ref=part, send_sem=self.send.at[i], recv_sem=self.recv.at[i], device_id=dev(self.side, *target), device_id_type=MESH_ID)


GATHER_COPIES = 22


def start(copies):
    for copy in copies:
        copy.start()


def arrive(copies):
    for copy in copies:
        copy.wait_recv()


def sent(copies):
    for copy in copies:
        copy.wait_send()


def my_rows(table, experts, me, offset):
    row = lax.broadcasted_iota(jnp.int32, (8, table.shape[-1]), 0)
    lane = lax.broadcasted_iota(jnp.int32, (8, table.shape[-1]), 1)
    pick = ((lane == offset + me) & (row == 0)) | ((lane == offset + experts + me) & (row == 1))
    return lax.dot_general(jnp.where(pick, 1.0, 0.0).astype(BF16), table, (((1,), (1,)), ((), ())), preferred_element_type=F32)


BLOCKS = 4


def backward_kernel(side, experts, dy_ref, u_ref, ub_ref, w13_ref, w2_ref, u_all, meta_all, du_ref, gw1, gw2, gw3, buf, w13t, w2t, tile, dout, acts, dtile, loc, tin, tout, sa, ra, sb, rb):
    me, y, x, core = place_of(side)
    partners = [dev(side, y, (x + k) % side, core) for k in range(1, side)]
    partners += [dev(side, (y + k) % side, x, core) for k in range(1, side)]
    partners += [dev(side, y, x, 1 - core)]
    greet(partners)
    dim = u_ref.shape[-1]
    width = w2_ref.shape[0]
    own_dy = pltpu.make_async_copy(dy_ref, buf.at[y, x, core], loc.at[0])
    own_u = pltpu.make_async_copy(u_ref, u_all.at[y, x, core], loc.at[1])
    own_dy.start()
    own_u.start()
    first = Gather(side, buf, dim // 2, sa, ra)
    second = Gather(side, u_all, dim // 2 + dim // 8, sb, rb)
    own_dy.wait()
    start(first.own)
    w13t[...] = w13_ref[...].T
    w2t[...] = w2_ref[...].T
    gw1[...] = jnp.zeros_like(gw1)
    gw2[...] = jnp.zeros_like(gw2)
    gw3[...] = jnp.zeros_like(gw3)
    own_u.wait()
    arrive(first.own)
    start(first.line)
    start(first.twin_own)
    arrive(first.line)
    start(first.relay)
    start(first.twin_line)
    start(second.own)
    arrive(first.relay)
    start(first.twin_far)
    arrive(first.twin_own + first.twin_line + first.twin_far)

    slots = du_ref.shape[1]
    group = du_ref.shape[0]
    rows = BLOCKS * slots
    steps = group // BLOCKS

    def fetch(g, slot):
        return pltpu.make_async_copy(ub_ref.at[pl.ds(g * rows, rows)], tile.at[slot], tin.at[slot])

    def put(g, slot):
        return pltpu.make_async_copy(dtile.at[slot], du_ref.at[pl.ds(g * BLOCKS, BLOCKS)], tout.at[slot])

    fetch(0, 0).start()
    spot = lax.broadcasted_iota(jnp.int32, (slots, 1), 0).astype(F32)

    def step(g, carry):
        slot = g % 2
        fetch(g, slot).wait()

        @pl.when(g + 1 < steps)
        def _():
            fetch(g + 1, 1 - slot).start()
        for j in range(BLOCKS):
            p = g * BLOCKS + j
            block = buf.at[p // (side * CORES), (p // CORES) % side, p % CORES]
            lines = my_rows(block[:, dim:], experts, me, 2 * experts)
            pick = jnp.where(lines[0:1] == spot, lines[1:2], 0.0).astype(BF16)
            dout[pl.ds(j * slots, slots), :] = jnp.dot(pick, block[:, :dim], preferred_element_type=F32).astype(BF16)
        pre = jnp.dot(tile[slot], w13_ref[...], preferred_element_type=F32).astype(BF16).astype(F32)
        pre_1, pre_3 = pre[:, :width], pre[:, width:]
        sigma = jax.nn.sigmoid(pre_1)
        silu_1 = pre_1 * sigma
        hid = (silu_1 * pre_3).astype(BF16)
        grad_hid = jnp.dot(dout[...], w2t[...], preferred_element_type=F32).astype(BF16).astype(F32)
        acts[:, :width] = (grad_hid * pre_3 * sigma * (1.0 + pre_1 * (1.0 - sigma))).astype(BF16)
        acts[:, width:] = (grad_hid * silu_1).astype(BF16)

        @pl.when(g >= 2)
        def _():
            put(g - 2, slot).wait()
        grad_in = jnp.dot(acts[...], w13t[...], preferred_element_type=F32).astype(BF16)
        dtile[slot] = grad_in.reshape(BLOCKS, slots, dim)
        put(g, slot).start()
        over = (((0,), (0,)), ((), ()))
        gw2[...] += lax.dot_general(hid, dout[...], over, preferred_element_type=F32)
        both = lax.dot_general(tile[slot], acts[...], over, preferred_element_type=F32)
        gw1[...] += both[:, :width]
        gw3[...] += both[:, width:]

        @pl.when(g == 1)
        def _():
            arrive(second.own)
            start(second.line)
            start(second.twin_own)

        @pl.when(g == 6)
        def _():
            arrive(second.line)
            start(second.relay)
            start(second.twin_line)
        return carry

    lax.fori_loop(0, steps, step, 0)
    meta_out = pltpu.make_async_copy(buf.at[:, :, :, :, pl.ds(dim, buf.shape[-1] - dim)], meta_all, loc.at[0])
    meta_out.start()
    put(steps - 2, steps % 2).wait()
    put(steps - 1, 1 - steps % 2).wait()
    arrive(second.relay)
    start(second.twin_far)
    arrive(second.twin_own + second.twin_line + second.twin_far)
    for gather in (first, second):
        sent(gather.own + gather.line + gather.relay + gather.twin_own + gather.twin_line + gather.twin_far)
    meta_out.wait()


def run_backward(dy_ext, u_a, saved, w13, w2, group):
    side = int(round((group // CORES) ** 0.5))
    rows, dim = u_a.shape
    wide = dy_ext.shape[1]
    slots = saved.shape[0] // group
    width = w2.shape[0]
    tall = BLOCKS * slots
    any_spec, vmem = pl.BlockSpec(memory_space=pl.ANY), pl.BlockSpec(memory_space=pltpu.VMEM)
    return pl.pallas_call(
        functools.partial(backward_kernel, side, group),
        out_shape=[
            jax.ShapeDtypeStruct((side, side, CORES, rows, dim), BF16),
            jax.ShapeDtypeStruct((side, side, CORES, rows, wide - dim), BF16),
            jax.ShapeDtypeStruct((group, slots, dim), BF16),
            jax.ShapeDtypeStruct((dim, width), F32),
            jax.ShapeDtypeStruct((width, dim), F32),
            jax.ShapeDtypeStruct((dim, width), F32),
        ],
        in_specs=[any_spec, vmem, any_spec, vmem, vmem],
        out_specs=[any_spec, any_spec, any_spec, vmem, vmem, vmem],
        scratch_shapes=[
            pltpu.VMEM((side, side, CORES, rows, wide), BF16),
            pltpu.VMEM((2 * width, dim), BF16),
            pltpu.VMEM((dim, width), BF16),
            pltpu.VMEM((2, tall, dim), BF16),
            pltpu.VMEM((tall, dim), BF16),
            pltpu.VMEM((tall, 2 * width), BF16),
            pltpu.VMEM((2, BLOCKS, slots, dim), BF16),
            pltpu.SemaphoreType.DMA((2,)),
            pltpu.SemaphoreType.DMA((2,)),
            pltpu.SemaphoreType.DMA((2,)),
        ] + [pltpu.SemaphoreType.DMA((GATHER_COPIES,))] * 4,
        compiler_params=pltpu.CompilerParams(collective_id=0, has_side_effects=True, vmem_limit_bytes=64000000),
    )(dy_ext, u_a, saved, w13, w2)


def combine_kernel(side, experts, offset, gated, forward, *refs):
    if forward:
        o_ref, base_ref, meta_ref, u_all, w13_ref, w2_ref, out_ref, fwd_ref, meta, r1l, r1r, ps_l, ps_r, p2l, p2r, loc_sem, s1, v1, s2, v2, utile, recv, otile, tin, tout = refs
    else:
        o_ref, base_ref, meta_ref, out_ref, meta, r1l, r1r, ps_l, ps_r, p2l, p2r, loc_sem, s1, v1, s2, v2 = refs
    me, y, x, core = place_of(side)
    peers = side * CORES
    q_row = x * CORES + core
    q_col = y * CORES + core
    half = o_ref.shape[-1] // 2
    slots = o_ref.shape[-2]
    moves = [(k, dc) for k in range(1, side) for dc in range(CORES)] + [(0, 1)]
    partners = [(y, (x + k) % side, (core + dc) % CORES) for k, dc in moves]
    partners += [((y + k) % side, x, (core + dc) % CORES) for k, dc in moves if k]
    greet([dev(side, *spot) for spot in partners])

    first = []
    for i, (k, dc) in enumerate(moves):
        xt, yt, ct = (x + k) % side, (y + k) % side, (core + dc) % CORES
        first.append(pltpu.make_async_remote_copy(src_ref=o_ref.at[:, xt, ct, :, pl.ds(0, half)], dst_ref=r1l.at[:, q_row], send_sem=s1.at[0, i], recv_sem=v1.at[0, i], device_id=dev(side, y, xt, ct), device_id_type=MESH_ID))
        first.append(pltpu.make_async_remote_copy(src_ref=o_ref.at[yt, :, ct, :, pl.ds(half, half)], dst_ref=r1r.at[:, q_col], send_sem=s1.at[1, i], recv_sem=v1.at[1, i], device_id=dev(side, yt, x, ct), device_id_type=MESH_ID))
    start(first)
    own_l = pltpu.make_async_copy(o_ref.at[:, x, core, :, pl.ds(0, half)], r1l.at[:, q_row], loc_sem.at[0])
    own_r = pltpu.make_async_copy(o_ref.at[y, :, core, :, pl.ds(half, half)], r1r.at[:, q_col], loc_sem.at[1])
    meta_in = pltpu.make_async_copy(meta_ref, meta, loc_sem.at[2])
    own_l.start()
    own_r.start()
    meta_in.start()
    meta_in.wait()

    if forward:
        width = w2_ref.shape[0]
        group = fwd_ref.shape[0]
        steps = group // BLOCKS
        tokens = u_all.shape[1]
        spot = lax.broadcasted_iota(jnp.int32, (slots, 1), 0).astype(F32)

        def fetch(g, slot):
            return pltpu.make_async_copy(u_all.at[pl.ds(g * BLOCKS, BLOCKS)], utile.at[slot], tin.at[slot])

        def put(g, slot):
            return pltpu.make_async_copy(otile.at[slot], fwd_ref.at[pl.ds(g * BLOCKS, BLOCKS)], tout.at[slot])

        fetch(0, 0).start()

        def step(g, carry):
            slot = g % 2
            fetch(g, slot).wait()

            @pl.when(g + 1 < steps)
            def _():
                fetch(g + 1, 1 - slot).start()
            for j in range(BLOCKS):
                p = g * BLOCKS + j
                lines = my_rows(meta[p // (side * CORES), (p // CORES) % side, p % CORES], experts, me, 0)
                pick = jnp.where(lines[0:1] == spot, 1.0, 0.0).astype(BF16)
                recv[pl.ds(j * slots, slots), :] = jnp.dot(pick, utile[slot, j], preferred_element_type=F32).astype(BF16)
            act = jnp.dot(recv[...], w13_ref[...], preferred_element_type=F32).astype(BF16).astype(F32)
            act_1, act_3 = act[:, :width], act[:, width:]
            hidden = (act_1 * jax.nn.sigmoid(act_1) * act_3).astype(BF16)

            @pl.when(g >= 2)
            def _():
                put(g - 2, slot).wait()
            otile[slot] = jnp.dot(hidden, w2_ref[...], preferred_element_type=F32).astype(BF16).reshape(BLOCKS, slots, 2 * half)
            put(g, slot).start()
            return carry

        lax.fori_loop(0, steps, step, 0)
        put(steps - 2, steps % 2).wait()
        put(steps - 1, 1 - steps % 2).wait()

    own_l.wait()
    own_r.wait()
    arrive(first)

    lane = lax.broadcasted_iota(jnp.int32, (1, slots), 1).astype(F32)
    row_ids = [y * peers + q for q in range(peers)]
    col_ids = [((q // CORES) * side + x) * CORES + q % CORES for q in range(peers)]

    def selector(ids):
        wide = meta.shape[-1]
        src = lax.broadcasted_iota(jnp.int32, (wide, wide), 0)
        dst = lax.broadcasted_iota(jnp.int32, (wide, wide), 1)
        hit = jnp.zeros((wide, wide), F32)
        for q, e in enumerate(ids):
            hit = jnp.where((src == offset + e) & (dst == q), 1.0, hit)
            hit = jnp.where((src == offset + experts + e) & (dst == peers + q), 1.0, hit)
        return hit.astype(BF16)

    sel_l, sel_r = selector(row_ids), selector(col_ids)

    def partial(block, sel, landed, sums, k):
        table = jnp.dot(block, sel, preferred_element_type=F32)
        weights = []
        for q in range(peers):
            scale = table[:, peers + q:peers + q + 1] if gated else 1.0
            weights.append(jnp.where(table[:, q:q + 1] == lane, scale, 0.0).astype(BF16))
        vals = landed[k].reshape(peers * slots, half)
        sums[k] = jnp.dot(jnp.concatenate(weights, axis=1), vals, preferred_element_type=F32)

    def sum_l(i):
        k = (y + i) % side
        partial(meta[k, x, core], sel_l, r1l, ps_l, k)

    def sum_r(i):
        k = (x + i) % side
        partial(meta[y, k, core], sel_r, r1r, ps_r, k)

    def send_l(i):
        yt = (y + i) % side
        return pltpu.make_async_remote_copy(src_ref=ps_l.at[yt], dst_ref=p2l.at[i], send_sem=s2.at[0, i], recv_sem=v2.at[0, i], device_id=dev(side, yt, x, core), device_id_type=MESH_ID)

    def send_r(i):
        xt = (x + i) % side
        return pltpu.make_async_remote_copy(src_ref=ps_r.at[xt], dst_ref=p2r.at[i], send_sem=s2.at[1, i], recv_sem=v2.at[1, i], device_id=dev(side, y, xt, core), device_id_type=MESH_ID)

    second = []
    for i in range(1, side):
        sum_l(i)
        if i > 1:
            second.append(send_r(i - 1))
            second[-1].start()
        sum_r(i)
        second.append(send_l(i))
        second[-1].start()
    sum_l(0)
    second.append(send_r(side - 1))
    second[-1].start()
    sum_r(0)
    sent(first)
    arrive(second)
    total_l = base_ref[:, :half].astype(F32) + ps_l[y]
    for i in range(1, side):
        total_l = total_l + p2l[i]
    out_ref[:, :half] = total_l.astype(BF16)
    total_r = base_ref[:, half:].astype(F32) + ps_r[x]
    for i in range(1, side):
        total_r = total_r + p2r[i]
    out_ref[:, half:] = total_r.astype(BF16)
    sent(second)


def run_combine(ident, out_slots, base, meta, offset, gated, extra=()):
    side = meta.shape[0]
    group, capacity, dim = out_slots.shape
    rows = base.shape[0]
    half = dim // 2
    peers = side * CORES
    cube = out_slots.reshape(side, side, CORES, capacity, dim)
    any_spec, vmem = pl.BlockSpec(memory_space=pl.ANY), pl.BlockSpec(memory_space=pltpu.VMEM)
    out_shape = [jax.ShapeDtypeStruct(base.shape, BF16)]
    in_specs = [any_spec, vmem, any_spec]
    out_specs = [vmem]
    scratch = [
        pltpu.VMEM(meta.shape, BF16),
        pltpu.VMEM((side, peers, capacity, half), BF16),
        pltpu.VMEM((side, peers, capacity, half), BF16),
        pltpu.VMEM((side, rows, half), F32),
        pltpu.VMEM((side, rows, half), F32),
        pltpu.VMEM((side, rows, half), F32),
        pltpu.VMEM((side, rows, half), F32),
        pltpu.SemaphoreType.DMA((3,)),
        pltpu.SemaphoreType.DMA((2, peers)),
        pltpu.SemaphoreType.DMA((2, peers)),
        pltpu.SemaphoreType.DMA((2, side)),
        pltpu.SemaphoreType.DMA((2, side)),
    ]
    if extra:
        in_specs += [any_spec, vmem, vmem]
        out_specs += [any_spec]
        out_shape += [jax.ShapeDtypeStruct(out_slots.shape, BF16)]
        scratch += [
            pltpu.VMEM((2, BLOCKS, rows, dim), BF16),
            pltpu.VMEM((BLOCKS * capacity, dim), BF16),
            pltpu.VMEM((2, BLOCKS, capacity, dim), BF16),
            pltpu.SemaphoreType.DMA((2,)),
            pltpu.SemaphoreType.DMA((2,)),
        ]
    return pl.pallas_call(
        functools.partial(combine_kernel, side, group, offset, gated, bool(extra)),
        out_shape=out_shape,
        in_specs=in_specs,
        out_specs=out_specs,
        scratch_shapes=scratch,
        compiler_params=pltpu.CompilerParams(collective_id=ident, has_side_effects=True, vmem_limit_bytes=64000000),
    )(cube, base, meta, *extra)


def solution(mesh):
    group = mesh.shape['expert']

    def local_step(x_a, x_b, dy_b, eid_a, slot_a, gate_a, eid_b, slot_b, gate_b, u_b, norm_1, norm_2, w_q, w_k, w_v, w_o, w_1, w_2, w_3):
        experts = w_1.shape[0] * group
        rows, model_dim = x_a.shape
        w1, w2, w3 = w_1[0], w_2[0], w_3[0]

        tables = slot_tables(eid_a, slot_a, gate_a, experts) + slot_tables(eid_b, slot_b, gate_b, experts)
        dy_ext = jnp.concatenate((dy_b,) + tables, axis=1)
        w13 = jnp.concatenate([w1, w3], axis=1)

        h_a = add_rows(x_a, attn_out(x_a, norm_1, w_q, w_k, w_v, w_o))
        u_a = rms_norm(h_a, norm_2)
        attn_val, attn_pull = jax.vjp(attn_out, x_b, norm_1, w_q, w_k, w_v, w_o)
        h_b = add_rows(x_b, attn_val)

        u_all, meta, grad_in, grad_w1, grad_w2, grad_w3 = run_backward(dy_ext, u_a, u_b[0], w13, w2, group)
        du, out_a = run_combine(1, grad_in, jnp.zeros_like(x_b), meta, 2 * experts, False, (u_all.reshape(group, rows, model_dim), w13, w2))
        y_a, = run_combine(2, out_a, h_a, meta, 0, True)

        _, norm_pull = jax.vjp(rms_norm, h_b, norm_2)
        dh_norm, g_n2 = norm_pull(du)
        dh = add_rows(dy_b, dh_norm)
        grad_x, g_n1, g_q, g_k, g_v, g_o = attn_pull(dh)
        dx_b = add_rows(dh, grad_x)
        grads = [g.astype(F32)[None] for g in (g_q, g_k, g_v, g_o, g_n1, g_n2)]
        return (y_a, dx_b, grad_w1[None], grad_w2[None], grad_w3[None], *grads)

    row_spec = P(('data', 'expert'), None)
    cube_spec = P(('data', 'expert'), None, None)
    quad_spec = P(('data', 'expert'), None, None, None)
    expert_spec = P('expert', None, None)
    in_specs = (row_spec, row_spec, row_spec, row_spec, row_spec, row_spec, row_spec, row_spec, row_spec, cube_spec, P(), P(), P(), P(), P(), P(), expert_spec, expert_spec, expert_spec)
    out_specs = (row_spec, row_spec, cube_spec, cube_spec, cube_spec, quad_spec, quad_spec, quad_spec, quad_spec, row_spec, row_spec)
    return jax.shard_map(local_step, mesh=mesh, in_specs=in_specs, out_specs=out_specs, check_vma=False)
```

```python
import functools

import jax
import jax.numpy as jnp
from jax import lax
from jax.experimental import pallas as pl
from jax.experimental.pallas import tpu as pltpu
from jax.sharding import PartitionSpec as P

NORM_EPS = 1e-6
CORES = 2
BF16 = jnp.bfloat16
F32 = jnp.float32
MESH_ID = pl.DeviceIdType.MESH


def slot_table(routes, experts):
    choices, rows = routes[0].shape
    columns = [part[...].astype(F32).T for part in routes]
    lane = lax.broadcasted_iota(jnp.int32, (rows, 4 * experts), 1).astype(F32)
    table = jnp.zeros(lane.shape, F32)
    for i in range(2):
        for j in range(choices):
            eid, slot, gate = [columns[3 * i + k][:, j:j + 1] for k in range(3)]
            spot = eid + 2.0 * i * experts
            table = jnp.where(lane == spot, slot + 1.0, table)
            table = jnp.where(lane == spot + experts, gate, table)
    return table.astype(BF16)


def place_of(side_x):
    me = lax.axis_index('expert')
    core = me % CORES
    return me, me // (CORES * side_x), (me // CORES) % side_x, core


def dev(side_x, yy, xx, cc):
    return {'expert': (yy * side_x + xx) * CORES + cc}


def greet(partners):
    barrier = pltpu.get_barrier_semaphore()
    for spot in partners:
        pl.semaphore_signal(barrier, inc=1, device_id=spot, device_id_type=MESH_ID)
    pl.semaphore_wait(barrier, len(partners))


class Gather:
    def __init__(self, side, buf, cut, send, recv):
        self.side, self.buf, self.send, self.recv = side, buf, send, recv
        _, self.y, self.x, self.core = place_of(side)
        width = buf.shape[-1]
        self.left, self.right = pl.ds(0, cut), pl.ds(cut, width - cut)
        self.count = 0
        y, x, c, side = self.y, self.x, self.core, self.side
        up, down, far = (y + 1) % side, (y + side - 1) % side, (y + 2) % side
        east, west, over = (x + 1) % side, (x + side - 1) % side, (x + 2) % side
        every = pl.ds(0, side)
        twin = 1 - c
        L, R = self.left, self.right
        self.own, self.line, self.relay = [], [], []
        for k in range(1, side):
            self.own.append([self.make((y, x, c, L), (y, (x + k) % side, c)), self.make((y, x, c, R), ((y + k) % side, x, c))])
        for k in range(side):
            xx, yy = (x + side - k) % side, (y + side - k) % side
            self.line.append([self.make((y, xx, c, L), (up, x, c)), self.make((yy, x, c, R), (y, east, c)),
                              self.make((y, xx, c, L), (down, x, c)), self.make((yy, x, c, R), (y, west, c))])
        for k in range(side):
            xx, yy = (x + side - k) % side, (y + side - k) % side
            if k < 2:
                self.relay.append([self.make((down, xx, c, L), (up, x, c)), self.make((yy, west, c, R), (y, east, c))])
            else:
                self.relay.append([self.make((up, xx, c, L), (down, x, c)), self.make((yy, east, c, R), (y, west, c))])
        self.twin_own = [self.make((y, every, c, L), (y, x, twin)), self.make((every, x, c, R), (y, x, twin))]
        self.twin_line = [self.make((up, every, c, L), (y, x, twin)), self.make((every, east, c, R), (y, x, twin)),
                          self.make((down, every, c, L), (y, x, twin)), self.make((every, west, c, R), (y, x, twin))]
        self.twin_far = [self.make((far, every, c, L), (y, x, twin)), self.make((every, over, c, R), (y, x, twin))]

    def owns(self):
        for k in (0, 2, 1):
            start(self.own[k])

    def lines(self):
        for k in (1, 3, 2):
            arrive(self.own[k - 1])
            start(self.line[k])
        start(self.twin_own)

    def relays(self, order):
        for k in order:
            arrive(self.line[k][:2] if k < 2 else self.line[k][2:])
            start(self.relay[k])

    def rest_of_lines(self):
        for k in (2, 3):
            arrive(self.line[k][:2])
        for k in (0, 1):
            arrive(self.line[k][2:])
        start(self.twin_line)

    def fars(self):
        for k in range(self.side):
            arrive(self.relay[k])
        start(self.twin_far)

    def finish(self):
        arrive(self.twin_own + self.twin_line + self.twin_far)

    def drain(self):
        sent(sum(self.own + self.line + self.relay, []) + self.twin_own + self.twin_line + self.twin_far)

    def make(self, spot, target):
        yy, xx, cc, cols = spot
        part = self.buf.at[yy, xx, cc, :, cols]
        i = self.count
        self.count += 1
        return pltpu.make_async_remote_copy(src_ref=part, dst_ref=part, send_sem=self.send.at[i], recv_sem=self.recv.at[i], device_id=dev(self.side, *target), device_id_type=MESH_ID)


GATHER_COPIES = 38


def start(copies):
    for copy in copies:
        copy.start()


def arrive(copies):
    for copy in copies:
        copy.wait_recv()


def sent(copies):
    for copy in copies:
        copy.wait_send()


def my_rows(table, experts, me, offset):
    row = lax.broadcasted_iota(jnp.int32, (8, table.shape[-1]), 0)
    lane = lax.broadcasted_iota(jnp.int32, (8, table.shape[-1]), 1)
    pick = ((lane == offset + me) & (row == 0)) | ((lane == offset + experts + me) & (row == 1))
    return lax.dot_general(jnp.where(pick, 1.0, 0.0).astype(BF16), table, (((1,), (1,)), ((), ())), preferred_element_type=F32)


def scaled_rows(wide, gain):
    scaled = wide * lax.rsqrt(jnp.mean(wide * wide, axis=-1, keepdims=True) + NORM_EPS)
    return (scaled * gain).astype(BF16)


def head_pair_probs(q_pair, k_head):
    tokens, head_dim = k_head.shape
    scores = lax.dot_general(q_pair, k_head, (((1,), (1,)), ((), ())), preferred_element_type=F32) * head_dim ** -0.5
    row = lax.broadcasted_iota(jnp.int32, (tokens, tokens), 0)
    col = lax.broadcasted_iota(jnp.int32, (tokens, tokens), 1)
    causal = row >= col
    scores = jnp.where(jnp.concatenate([causal, causal], axis=0), scores, -1e30)
    weights = jnp.exp(scores - jnp.max(scores, axis=-1, keepdims=True))
    return weights / jnp.sum(weights, axis=-1, keepdims=True)


def attention_rows(x_ref, gain, wq, wk, wv, wo, head_dim, q_s, k_s, v_s, ctx_s, normed_s):
    tokens = x_ref.shape[0]
    normed_s[...] = scaled_rows(x_ref[...].astype(F32), gain)
    q_s[...] = jnp.dot(normed_s[...], wq[...], preferred_element_type=F32).astype(BF16)
    k_s[...] = jnp.dot(normed_s[...], wk[...], preferred_element_type=F32).astype(BF16)
    v_s[...] = jnp.dot(normed_s[...], wv[...], preferred_element_type=F32).astype(BF16)
    pack = 2 * head_dim

    def pair(m, carry):
        k_two = k_s[:, pl.ds(m * pack, pack)]
        v_two = v_s[:, pl.ds(m * pack, pack)]
        for j in range(2):
            cols = pl.ds((2 * m + j) * pack, pack)
            q_two = q_s[:, cols]
            q_pair = jnp.concatenate([q_two[:, :head_dim], q_two[:, head_dim:]], axis=0)
            k_head = k_two[:, j * head_dim:(j + 1) * head_dim]
            v_head = v_two[:, j * head_dim:(j + 1) * head_dim]
            probs = head_pair_probs(q_pair, k_head).astype(BF16)
            ctx = jnp.dot(probs, v_head, preferred_element_type=F32).astype(BF16)
            ctx_s[:, cols] = jnp.concatenate([ctx[:tokens], ctx[tokens:]], axis=1)
        return carry

    lax.fori_loop(0, k_s.shape[1] // pack, pair, 0)
    return jnp.dot(ctx_s[...], wo[...], preferred_element_type=F32)


NT = (((1,), (1,)), ((), ()))
TN = (((0,), (0,)), ((), ()))


def norm_pull(wide, gain, grad):
    scale = lax.rsqrt(jnp.mean(wide * wide, axis=-1, keepdims=True) + NORM_EPS)
    grad_gain = jnp.sum(grad * (wide * scale), axis=0, keepdims=True)
    lifted = grad * gain
    pull = lifted * scale - wide * (scale * scale * scale * jnp.mean(lifted * wide, axis=-1, keepdims=True))
    return pull.astype(BF16), grad_gain.astype(BF16).astype(F32)


def attention_backward(head_dim, x_ref, dy_ref, du_ref, gains_ref, wq, wk, wv, wo, dx_ref, gq, gk, gv, go, gn, q_s, k_s, v_s, ctx_s, normed_s, dctx_s, dq_s, dk_s, dv_s, dh_s):
    tokens = x_ref.shape[0]
    gain_1, gain_2 = gains_ref[0:1].astype(F32), gains_ref[1:2].astype(F32)
    attn = attention_rows(x_ref, gain_1, wq, wk, wv, wo, head_dim, q_s, k_s, v_s, ctx_s, normed_s)
    h = (x_ref[...].astype(F32) + attn.astype(BF16).astype(F32)).astype(BF16)
    pulled, grad_gain = norm_pull(h.astype(F32), gain_2, du_ref[...].astype(F32))
    gn[1:2, :] = grad_gain
    dh_s[...] = (dy_ref[...].astype(F32) + pulled.astype(F32)).astype(BF16)
    dctx_s[...] = lax.dot_general(dh_s[...], wo[...], NT, preferred_element_type=F32).astype(BF16)
    go[...] = lax.dot_general(ctx_s[...], dh_s[...], TN, preferred_element_type=F32).astype(BF16)
    pack = 2 * head_dim

    def stack(two):
        return jnp.concatenate([two[:, :head_dim], two[:, head_dim:]], axis=0)

    def pair(m, carry):
        tile = pl.ds(m * pack, pack)
        k_two, v_two = k_s[:, tile], v_s[:, tile]
        dk, dv = [], []
        for j in range(2):
            cols = pl.ds((2 * m + j) * pack, pack)
            q_pair, dctx_pair = stack(q_s[:, cols]), stack(dctx_s[:, cols])
            k_head = k_two[:, j * head_dim:(j + 1) * head_dim]
            v_head = v_two[:, j * head_dim:(j + 1) * head_dim]
            probs = head_pair_probs(q_pair, k_head)
            dprobs = lax.dot_general(dctx_pair, v_head, NT, preferred_element_type=F32).astype(BF16).astype(F32)
            dv.append(lax.dot_general(probs.astype(BF16), dctx_pair, TN, preferred_element_type=F32).astype(BF16))
            dscores = probs * (dprobs - jnp.sum(dprobs * probs, axis=-1, keepdims=True))
            dscores = (dscores * head_dim ** -0.5).astype(BF16)
            dq = jnp.dot(dscores, k_head, preferred_element_type=F32).astype(BF16)
            dq_s[:, cols] = jnp.concatenate([dq[:tokens], dq[tokens:]], axis=1)
            dk.append(lax.dot_general(dscores, q_pair, TN, preferred_element_type=F32).astype(BF16))
        dk_s[:, tile] = jnp.concatenate(dk, axis=1)
        dv_s[:, tile] = jnp.concatenate(dv, axis=1)
        return carry

    lax.fori_loop(0, k_s.shape[1] // pack, pair, 0)
    for grad, source in ((gq, dq_s), (gk, dk_s), (gv, dv_s)):
        grad[...] = lax.dot_general(normed_s[...], source[...], TN, preferred_element_type=F32).astype(BF16)
    dnormed = sum(lax.dot_general(source[...], weight[...], NT, preferred_element_type=F32) for source, weight in ((dq_s, wq), (dk_s, wk), (dv_s, wv)))
    pulled, grad_gain = norm_pull(x_ref[...].astype(F32), gain_1, dnormed.astype(BF16).astype(F32))
    gn[0:1, :] = grad_gain
    dx_ref[...] = (dh_s[...].astype(F32) + pulled.astype(F32)).astype(BF16)


BLOCKS = 4


def backward_kernel(side, experts, head_dim, dy_ref, x_ref, eid_a, slot_a, gate_a, eid_b, slot_b, gate_b, ub_ref, w1_ref, w2_ref, w3_ref, gains_ref, wq_ref, wk_ref, wv_ref, wo_ref, u_all, meta_all, du_ref, gw1, gw2, gw3, h_ref, buf, w13, w13t, w2t, tile, dout, acts, dtile, u_ref, loc, tin, tout, sa, ra, sb, rb):
    me, y, x, core = place_of(side)
    partners = [dev(side, y, (x + k) % side, core) for k in range(1, side)]
    partners += [dev(side, (y + k) % side, x, core) for k in range(1, side)]
    partners += [dev(side, y, x, 1 - core)]
    dim = x_ref.shape[-1]
    width = w2_ref.shape[0]
    own_dy = pltpu.make_async_copy(dy_ref, buf.at[y, x, core, :, pl.ds(0, dim)], loc.at[0])
    own_u = pltpu.make_async_copy(u_ref, u_all.at[y, x, core], loc.at[1])
    greet(partners)
    own_dy.start()
    buf[y, x, core, :, dim:] = slot_table((eid_a, slot_a, gate_a, eid_b, slot_b, gate_b), experts)
    first = Gather(side, buf, dim // 2, sa, ra)
    second = Gather(side, u_all, dim // 2 + dim // 8, sb, rb)
    own_dy.wait()
    first.owns()
    start(first.line[0])
    tokens = x_ref.shape[0]
    kv = wk_ref.shape[1]
    attn = attention_rows(x_ref, gains_ref[0:1].astype(F32), wq_ref, wk_ref, wv_ref, wo_ref, head_dim, acts.at[pl.ds(0, tokens)], dout.at[pl.ds(0, tokens), pl.ds(0, kv)], dout.at[pl.ds(0, tokens), pl.ds(kv, kv)], acts.at[pl.ds(tokens, tokens)], dout.at[pl.ds(tokens, tokens)])
    h_ref[...] = (x_ref[...].astype(F32) + attn.astype(BF16).astype(F32)).astype(BF16)
    u_ref[...] = scaled_rows(h_ref[...].astype(F32), gains_ref[1:2].astype(F32))
    own_u.start()
    first.lines()
    w13[:, :width] = w1_ref[...]
    w13[:, width:] = w3_ref[...]
    w13t[...] = w13[...].T
    w2t[...] = w2_ref[...].T
    gw1[...] = jnp.zeros_like(gw1)
    gw2[...] = jnp.zeros_like(gw2)
    gw3[...] = jnp.zeros_like(gw3)
    own_u.wait()
    second.owns()
    first.relays((0, 1, 3, 2))
    start(second.line[0])
    first.rest_of_lines()
    arrive(first.twin_own + first.twin_line)

    slots = du_ref.shape[1]
    group = du_ref.shape[0]
    rows = BLOCKS * slots
    steps = group // BLOCKS

    def turn(g):
        far = jnp.where(g < 3, 0, jnp.where(g < 6, 1, g - 6))
        near = jnp.where(g < 3, g, jnp.where(g < 6, g - 3, 3))
        near = near + jnp.where(near == 2, 1, 0) - jnp.where(near == 3, 1, 0)
        pair = x // 2
        return ((y + near) % side) * (side // 2) + jnp.where(far == 1, 1 - pair, pair)

    def fetch(g, slot):
        return pltpu.make_async_copy(ub_ref.at[pl.ds(turn(g) * rows, rows)], tile.at[slot], tin.at[slot])

    def put(g, slot):
        return pltpu.make_async_copy(dtile.at[slot], du_ref.at[pl.ds(turn(g) * BLOCKS, BLOCKS)], tout.at[slot])

    fetch(0, 0).start()
    spot = lax.broadcasted_iota(jnp.int32, (slots, 1), 0).astype(F32) + 1.0

    def step(g, carry):
        slot = g % 2

        @pl.when(g == 1)
        def _():
            second.lines()

        @pl.when(g == 2)
        def _():
            first.fars()

        @pl.when(g == 3)
        def _():
            arrive(first.twin_far)

        @pl.when(g == 6)
        def _():
            second.relays((0, 1))

        @pl.when(g == 7)
        def _():
            second.relays((3,))
        fetch(g, slot).wait()

        @pl.when(g + 1 < steps)
        def _():
            fetch(g + 1, 1 - slot).start()
        for j in range(BLOCKS):
            p = turn(g) * BLOCKS + j
            block = buf.at[p // (side * CORES), (p // CORES) % side, p % CORES]
            lines = my_rows(block[:, dim:], experts, me, 2 * experts)
            pick = jnp.where(lines[0:1] == spot, lines[1:2], 0.0).astype(BF16)
            dout[pl.ds(j * slots, slots), :] = jnp.dot(pick, block[:, :dim], preferred_element_type=F32).astype(BF16)
        pre = jnp.dot(tile[slot], w13[...], preferred_element_type=F32).astype(BF16).astype(F32)
        pre_1, pre_3 = pre[:, :width], pre[:, width:]
        sigma = jax.nn.sigmoid(pre_1)
        silu_1 = pre_1 * sigma
        hid = (silu_1 * pre_3).astype(BF16)
        grad_hid = jnp.dot(dout[...], w2t[...], preferred_element_type=F32).astype(BF16).astype(F32)
        acts[:, :width] = (grad_hid * pre_3 * sigma * (1.0 + pre_1 * (1.0 - sigma))).astype(BF16)
        acts[:, width:] = (grad_hid * silu_1).astype(BF16)

        @pl.when(g >= 2)
        def _():
            put(g - 2, slot).wait()
        grad_in = jnp.dot(acts[...], w13t[...], preferred_element_type=F32).astype(BF16)
        dtile[slot] = grad_in.reshape(BLOCKS, slots, dim)
        put(g, slot).start()
        over = (((0,), (0,)), ((), ()))
        gw2[...] += lax.dot_general(hid, dout[...], over, preferred_element_type=F32)
        both = lax.dot_general(tile[slot], acts[...], over, preferred_element_type=F32)
        gw1[...] += both[:, :width]
        gw3[...] += both[:, width:]
        return carry

    lax.fori_loop(0, steps, step, 0)
    second.relays((2,))
    second.rest_of_lines()
    second.fars()
    meta_out = pltpu.make_async_copy(buf.at[:, :, :, :, pl.ds(dim, buf.shape[-1] - dim)], meta_all, loc.at[0])
    meta_out.start()
    put(steps - 2, steps % 2).wait()
    put(steps - 1, 1 - steps % 2).wait()
    second.finish()
    first.drain()
    second.drain()
    meta_out.wait()


def run_backward(dy, x_a, routes, saved, weights, head_dim, group):
    side = int(round((group // CORES) ** 0.5))
    rows, dim = x_a.shape
    wide = dim + 4 * group
    slots = saved.shape[0] // group
    width = weights[1].shape[0]
    tall = BLOCKS * slots
    any_spec, vmem = pl.BlockSpec(memory_space=pl.ANY), pl.BlockSpec(memory_space=pltpu.VMEM)
    return pl.pallas_call(
        functools.partial(backward_kernel, side, group, head_dim),
        out_shape=[
            jax.ShapeDtypeStruct((side, side, CORES, rows, dim), BF16),
            jax.ShapeDtypeStruct((side, side, CORES, rows, wide - dim), BF16),
            jax.ShapeDtypeStruct((group, slots, dim), BF16),
            jax.ShapeDtypeStruct((dim, width), F32),
            jax.ShapeDtypeStruct((width, dim), F32),
            jax.ShapeDtypeStruct((dim, width), F32),
            jax.ShapeDtypeStruct((rows, dim), BF16),
        ],
        in_specs=[any_spec, vmem] + [vmem] * len(routes) + [any_spec] + [vmem] * len(weights),
        out_specs=[any_spec, any_spec, any_spec, vmem, vmem, vmem, vmem],
        scratch_shapes=[
            pltpu.VMEM((side, side, CORES, rows, wide), BF16),
            pltpu.VMEM((dim, 2 * width), BF16),
            pltpu.VMEM((2 * width, dim), BF16),
            pltpu.VMEM((dim, width), BF16),
            pltpu.VMEM((2, tall, dim), BF16),
            pltpu.VMEM((tall, dim), BF16),
            pltpu.VMEM((tall, 2 * width), BF16),
            pltpu.VMEM((2, BLOCKS, slots, dim), BF16),
            pltpu.VMEM((rows, dim), BF16),
            pltpu.SemaphoreType.DMA((2,)),
            pltpu.SemaphoreType.DMA((2,)),
            pltpu.SemaphoreType.DMA((2,)),
        ] + [pltpu.SemaphoreType.DMA((GATHER_COPIES,))] * 4,
        compiler_params=pltpu.CompilerParams(collective_id=0, has_side_effects=True, vmem_limit_bytes=64000000),
    )(dy, x_a, *routes, saved, *weights)


def combine_kernel(side, experts, offset, gated, forward, head_dim, *refs):
    if forward:
        o_ref, base_ref, meta_ref, u_all, w1_ref, w2_ref, w3_ref, out_ref, fwd_ref, meta, r1l, r1r, ps_l, ps_r, p2l, p2r, loc_sem, s1, v1, s2, v2, utile, recv, otile, w13, tin, tout = refs
    else:
        o_ref, base_ref, meta_ref = refs[:3]
        attention_refs = refs[3:11] + refs[12:18]
        attention_scratch = refs[-10:]
        out_ref = refs[11]
        meta, r1l, r1r, ps_l, ps_r, p2l, p2r, loc_sem, s1, v1, s2, v2 = refs[18:-10]
    me, y, x, core = place_of(side)
    peers = side * CORES
    q_row = x * CORES + core
    q_col = y * CORES + core
    half = o_ref.shape[-1] // 2
    slots = o_ref.shape[-2]
    moves = [(k, dc) for k in range(1, side) for dc in range(CORES)] + [(0, 1)]
    partners = [(y, (x + k) % side, (core + dc) % CORES) for k, dc in moves]
    partners += [((y + k) % side, x, (core + dc) % CORES) for k, dc in moves if k]
    greet([dev(side, *spot) for spot in partners])

    first = []
    for i, (k, dc) in enumerate(moves):
        xt, yt, ct = (x + k) % side, (y + k) % side, (core + dc) % CORES
        first.append(pltpu.make_async_remote_copy(src_ref=o_ref.at[:, xt, ct, :, pl.ds(0, half)], dst_ref=r1l.at[:, q_row], send_sem=s1.at[0, i], recv_sem=v1.at[0, i], device_id=dev(side, y, xt, ct), device_id_type=MESH_ID))
        first.append(pltpu.make_async_remote_copy(src_ref=o_ref.at[yt, :, ct, :, pl.ds(half, half)], dst_ref=r1r.at[:, q_col], send_sem=s1.at[1, i], recv_sem=v1.at[1, i], device_id=dev(side, yt, x, ct), device_id_type=MESH_ID))
    start(first)
    own_l = pltpu.make_async_copy(o_ref.at[:, x, core, :, pl.ds(0, half)], r1l.at[:, q_row], loc_sem.at[0])
    own_r = pltpu.make_async_copy(o_ref.at[y, :, core, :, pl.ds(half, half)], r1r.at[:, q_col], loc_sem.at[1])
    meta_in = pltpu.make_async_copy(meta_ref, meta, loc_sem.at[2])
    own_l.start()
    own_r.start()
    meta_in.start()
    meta_in.wait()

    if forward:
        width = w2_ref.shape[0]
        group = fwd_ref.shape[0]
        steps = group // BLOCKS
        tokens = u_all.shape[1]
        spot = lax.broadcasted_iota(jnp.int32, (slots, 1), 0).astype(F32) + 1.0

        def fetch(g, slot):
            return pltpu.make_async_copy(u_all.at[pl.ds(g * BLOCKS, BLOCKS)], utile.at[slot], tin.at[slot])

        def put(g, slot):
            return pltpu.make_async_copy(otile.at[slot], fwd_ref.at[pl.ds(g * BLOCKS, BLOCKS)], tout.at[slot])

        fetch(0, 0).start()
        w13[:, :width] = w1_ref[...]
        w13[:, width:] = w3_ref[...]

        def step(g, carry):
            slot = g % 2
            fetch(g, slot).wait()

            @pl.when(g + 1 < steps)
            def _():
                fetch(g + 1, 1 - slot).start()
            for j in range(BLOCKS):
                p = g * BLOCKS + j
                lines = my_rows(meta[p // (side * CORES), (p // CORES) % side, p % CORES], experts, me, 0)
                pick = jnp.where(lines[0:1] == spot, 1.0, 0.0).astype(BF16)
                recv[pl.ds(j * slots, slots), :] = jnp.dot(pick, utile[slot, j], preferred_element_type=F32).astype(BF16)
            act = jnp.dot(recv[...], w13[...], preferred_element_type=F32).astype(BF16).astype(F32)
            act_1, act_3 = act[:, :width], act[:, width:]
            hidden = (act_1 * jax.nn.sigmoid(act_1) * act_3).astype(BF16)

            @pl.when(g >= 2)
            def _():
                put(g - 2, slot).wait()
            otile[slot] = jnp.dot(hidden, w2_ref[...], preferred_element_type=F32).astype(BF16).reshape(BLOCKS, slots, 2 * half)
            put(g, slot).start()
            return carry

        lax.fori_loop(0, steps, step, 0)
        put(steps - 2, steps % 2).wait()
        put(steps - 1, 1 - steps % 2).wait()
    else:
        attention_backward(head_dim, *attention_refs, *attention_scratch)

    own_l.wait()
    own_r.wait()
    arrive(first)

    lane = lax.broadcasted_iota(jnp.int32, (1, slots), 1).astype(F32) + 1.0
    row_ids = [y * peers + q for q in range(peers)]
    col_ids = [((q // CORES) * side + x) * CORES + q % CORES for q in range(peers)]

    def selector(ids):
        wide = meta.shape[-1]
        src = lax.broadcasted_iota(jnp.int32, (wide, wide), 0)
        dst = lax.broadcasted_iota(jnp.int32, (wide, wide), 1)
        hit = jnp.zeros((wide, wide), F32)
        for q, e in enumerate(ids):
            hit = jnp.where((src == offset + e) & (dst == q), 1.0, hit)
            hit = jnp.where((src == offset + experts + e) & (dst == peers + q), 1.0, hit)
        return hit.astype(BF16)

    sel_l, sel_r = selector(row_ids), selector(col_ids)

    def partial(block, sel, landed, sums, k):
        table = jnp.dot(block, sel, preferred_element_type=F32)
        weights = []
        for q in range(peers):
            scale = table[:, peers + q:peers + q + 1] if gated else 1.0
            weights.append(jnp.where(table[:, q:q + 1] == lane, scale, 0.0).astype(BF16))
        vals = landed[k].reshape(peers * slots, half)
        sums[k] = jnp.dot(jnp.concatenate(weights, axis=1), vals, preferred_element_type=F32)

    def sum_l(i):
        k = (y + i) % side
        partial(meta[k, x, core], sel_l, r1l, ps_l, k)

    def sum_r(i):
        k = (x + i) % side
        partial(meta[y, k, core], sel_r, r1r, ps_r, k)

    def send_l(i):
        yt = (y + i) % side
        return pltpu.make_async_remote_copy(src_ref=ps_l.at[yt], dst_ref=p2l.at[i], send_sem=s2.at[0, i], recv_sem=v2.at[0, i], device_id=dev(side, yt, x, core), device_id_type=MESH_ID)

    def send_r(i):
        xt = (x + i) % side
        return pltpu.make_async_remote_copy(src_ref=ps_r.at[xt], dst_ref=p2r.at[i], send_sem=s2.at[1, i], recv_sem=v2.at[1, i], device_id=dev(side, y, xt, core), device_id_type=MESH_ID)

    second = []
    for i in range(1, side):
        sum_l(i)
        if i > 1:
            second.append(send_r(i - 1))
            second[-1].start()
        sum_r(i)
        second.append(send_l(i))
        second[-1].start()
    sum_l(0)
    second.append(send_r(side - 1))
    second[-1].start()
    sum_r(0)
    sent(first)
    arrive(second)
    total_l = base_ref[:, :half].astype(F32) + ps_l[y]
    for i in range(1, side):
        total_l = total_l + p2l[i]
    out_ref[:, :half] = total_l.astype(BF16)
    total_r = base_ref[:, half:].astype(F32) + ps_r[x]
    for i in range(1, side):
        total_r = total_r + p2r[i]
    out_ref[:, half:] = total_r.astype(BF16)
    sent(second)


def run_combine(ident, out_slots, base, meta, offset, gated, forward, head_dim, extra):
    side = meta.shape[0]
    group, capacity, dim = out_slots.shape
    rows = base.shape[0]
    half = dim // 2
    peers = side * CORES
    cube = out_slots.reshape(side, side, CORES, capacity, dim)
    any_spec, vmem = pl.BlockSpec(memory_space=pl.ANY), pl.BlockSpec(memory_space=pltpu.VMEM)
    out_shape = [jax.ShapeDtypeStruct(base.shape, BF16)]
    in_specs = [any_spec, vmem, any_spec]
    out_specs = [vmem]
    scratch = [
        pltpu.VMEM(meta.shape, BF16),
        pltpu.VMEM((side, peers, capacity, half), BF16),
        pltpu.VMEM((side, peers, capacity, half), BF16),
        pltpu.VMEM((side, rows, half), F32),
        pltpu.VMEM((side, rows, half), F32),
        pltpu.VMEM((side, rows, half), F32),
        pltpu.VMEM((side, rows, half), F32),
        pltpu.SemaphoreType.DMA((3,)),
        pltpu.SemaphoreType.DMA((2, peers)),
        pltpu.SemaphoreType.DMA((2, peers)),
        pltpu.SemaphoreType.DMA((2, side)),
        pltpu.SemaphoreType.DMA((2, side)),
    ]
    if forward:
        in_specs += [any_spec, vmem, vmem, vmem]
        out_specs += [any_spec]
        out_shape += [jax.ShapeDtypeStruct(out_slots.shape, BF16)]
        scratch += [
            pltpu.VMEM((2, BLOCKS, rows, dim), BF16),
            pltpu.VMEM((BLOCKS * capacity, dim), BF16),
            pltpu.VMEM((2, BLOCKS, capacity, dim), BF16),
            pltpu.VMEM((dim, 2 * extra[2].shape[0]), BF16),
            pltpu.SemaphoreType.DMA((2,)),
            pltpu.SemaphoreType.DMA((2,)),
        ]
    else:
        in_specs += [vmem] * len(extra)
        out_specs += [vmem] * 6
        full, kv = extra[4].shape[1], extra[5].shape[1]
        out_shape += [jax.ShapeDtypeStruct(base.shape, BF16)] + [jax.ShapeDtypeStruct(part.shape, BF16) for part in extra[4:]] + [jax.ShapeDtypeStruct((2, dim), F32)]
        scratch += [pltpu.VMEM((rows, cols), BF16) for cols in (full, kv, kv, full, dim, full, full, kv, kv, dim)]
    return pl.pallas_call(
        functools.partial(combine_kernel, side, group, offset, gated, forward, head_dim),
        out_shape=out_shape,
        in_specs=in_specs,
        out_specs=out_specs,
        scratch_shapes=scratch,
        compiler_params=pltpu.CompilerParams(collective_id=ident, has_side_effects=True, vmem_limit_bytes=64000000),
    )(cube, base, meta, *extra)


def solution(mesh):
    group = mesh.shape['expert']

    def local_step(x_a, x_b, dy_b, eid_a, slot_a, gate_a, eid_b, slot_b, gate_b, u_b, norm_1, norm_2, w_q, w_k, w_v, w_o, w_1, w_2, w_3):
        experts = w_1.shape[0] * group
        rows, model_dim = x_a.shape
        w1, w2, w3 = w_1[0], w_2[0], w_3[0]

        head_dim = w_q.shape[2]
        gains = jnp.stack([norm_1, norm_2])
        routes = tuple(part.T for part in (eid_a, slot_a, gate_a, eid_b, slot_b, gate_b))
        flat = (w_q.reshape(model_dim, -1), w_k.reshape(model_dim, -1), w_v.reshape(model_dim, -1), w_o.reshape(-1, model_dim))

        u_all, meta, grad_in, grad_w1, grad_w2, grad_w3, h_a = run_backward(dy_b, x_a, routes, u_b[0], (w1, w2, w3, gains) + flat, head_dim, group)
        du, out_a = run_combine(1, grad_in, jnp.zeros_like(x_b), meta, 2 * experts, False, True, head_dim, (u_all.reshape(group, rows, model_dim), w1, w2, w3))
        y_a, dx_b, g_q, g_k, g_v, g_o, g_n = run_combine(2, out_a, h_a, meta, 0, True, False, head_dim, (x_b, dy_b, du, gains) + flat)
        grads = tuple(g.reshape(w.shape).astype(F32)[None] for g, w in ((g_q, w_q), (g_k, w_k), (g_v, w_v), (g_o, w_o))) + (g_n[0:1], g_n[1:2])
        return (y_a, dx_b, grad_w1[None], grad_w2[None], grad_w3[None], *grads)

    row_spec = P(('data', 'expert'), None)
    cube_spec = P(('data', 'expert'), None, None)
    quad_spec = P(('data', 'expert'), None, None, None)
    expert_spec = P('expert', None, None)
    in_specs = (row_spec, row_spec, row_spec, row_spec, row_spec, row_spec, row_spec, row_spec, row_spec, cube_spec, P(), P(), P(), P(), P(), P(), expert_spec, expert_spec, expert_spec)
    out_specs = (row_spec, row_spec, cube_spec, cube_spec, cube_spec, quad_spec, quad_spec, quad_spec, quad_spec, row_spec, row_spec)
    return jax.shard_map(local_step, mesh=mesh, in_specs=in_specs, out_specs=out_specs, check_vma=False)
```

```python
import functools

import jax
import jax.numpy as jnp
from jax import lax
from jax.experimental import pallas as pl
from jax.experimental.pallas import tpu as pltpu
from jax.sharding import PartitionSpec as P

NORM_EPS = 1e-6
CORES = 2
BF16 = jnp.bfloat16
F32 = jnp.float32
MESH_ID = pl.DeviceIdType.MESH


def slot_table(routes, experts):
    choices, rows = routes[0].shape
    columns = [part[...].astype(F32).T for part in routes]
    lane = lax.broadcasted_iota(jnp.int32, (rows, 4 * experts), 1).astype(F32)
    table = jnp.zeros(lane.shape, F32)
    for i in range(2):
        for j in range(choices):
            eid, slot, gate = [columns[3 * i + k][:, j:j + 1] for k in range(3)]
            spot = eid + 2.0 * i * experts
            table = jnp.where(lane == spot, slot + 1.0, table)
            table = jnp.where(lane == spot + experts, gate, table)
    return table.astype(BF16)


def place_of(side_x):
    me = lax.axis_index('expert')
    core = me % CORES
    return me, me // (CORES * side_x), (me // CORES) % side_x, core


def dev(side_x, yy, xx, cc):
    return {'expert': (yy * side_x + xx) * CORES + cc}


def greet(partners):
    barrier = pltpu.get_barrier_semaphore()
    for spot in partners:
        pl.semaphore_signal(barrier, inc=1, device_id=spot, device_id_type=MESH_ID)
    pl.semaphore_wait(barrier, len(partners))


class Gather:
    def __init__(self, side, buf, cut, send, recv):
        self.side, self.buf, self.send, self.recv = side, buf, send, recv
        _, self.y, self.x, self.core = place_of(side)
        width = buf.shape[-1]
        self.left, self.right = pl.ds(0, cut), pl.ds(cut, width - cut)
        self.count = 0
        y, x, c, side = self.y, self.x, self.core, self.side
        up, down, far = (y + 1) % side, (y + side - 1) % side, (y + 2) % side
        east, west, over = (x + 1) % side, (x + side - 1) % side, (x + 2) % side
        every = pl.ds(0, side)
        twin = 1 - c
        L, R = self.left, self.right
        self.own, self.line, self.relay = [], [], []
        for k in range(1, side):
            self.own.append([self.make((y, x, c, L), (y, (x + k) % side, c)), self.make((y, x, c, R), ((y + k) % side, x, c))])
        for k in range(side):
            xx, yy = (x + side - k) % side, (y + side - k) % side
            self.line.append([self.make((y, xx, c, L), (up, x, c)), self.make((yy, x, c, R), (y, east, c)),
                              self.make((y, xx, c, L), (down, x, c)), self.make((yy, x, c, R), (y, west, c))])
        for k in range(side):
            xx, yy = (x + side - k) % side, (y + side - k) % side
            if k < 2:
                self.relay.append([self.make((down, xx, c, L), (up, x, c)), self.make((yy, west, c, R), (y, east, c))])
            else:
                self.relay.append([self.make((up, xx, c, L), (down, x, c)), self.make((yy, east, c, R), (y, west, c))])
        self.twin_own = [self.make((y, every, c, L), (y, x, twin)), self.make((every, x, c, R), (y, x, twin))]
        self.twin_line = [self.make((up, every, c, L), (y, x, twin)), self.make((every, east, c, R), (y, x, twin)),
                          self.make((down, every, c, L), (y, x, twin)), self.make((every, west, c, R), (y, x, twin))]
        self.twin_far = [self.make((far, every, c, L), (y, x, twin)), self.make((every, over, c, R), (y, x, twin))]

    def owns(self):
        for k in (0, 2, 1):
            start(self.own[k])

    def lines(self):
        for k in (1, 3, 2):
            arrive(self.own[k - 1])
            start(self.line[k])
        start(self.twin_own)

    def relays(self, order):
        for k in order:
            arrive(self.line[k][:2] if k < 2 else self.line[k][2:])
            start(self.relay[k])

    def rest_of_lines(self):
        for k in (2, 3):
            arrive(self.line[k][:2])
        for k in (0, 1):
            arrive(self.line[k][2:])
        start(self.twin_line)

    def fars(self):
        for k in range(self.side):
            arrive(self.relay[k])
        start(self.twin_far)

    def finish(self):
        arrive(self.twin_own + self.twin_line + self.twin_far)

    def drain(self):
        sent(sum(self.own + self.line + self.relay, []) + self.twin_own + self.twin_line + self.twin_far)

    def make(self, spot, target):
        yy, xx, cc, cols = spot
        part = self.buf.at[yy, xx, cc, :, cols]
        i = self.count
        self.count += 1
        return pltpu.make_async_remote_copy(src_ref=part, dst_ref=part, send_sem=self.send.at[i], recv_sem=self.recv.at[i], device_id=dev(self.side, *target), device_id_type=MESH_ID)


GATHER_COPIES = 38


def start(copies):
    for copy in copies:
        copy.start()


def arrive(copies):
    for copy in copies:
        copy.wait_recv()


def sent(copies):
    for copy in copies:
        copy.wait_send()


def my_rows(table, experts, me, offset):
    row = lax.broadcasted_iota(jnp.int32, (8, table.shape[-1]), 0)
    lane = lax.broadcasted_iota(jnp.int32, (8, table.shape[-1]), 1)
    pick = ((lane == offset + me) & (row == 0)) | ((lane == offset + experts + me) & (row == 1))
    return lax.dot_general(jnp.where(pick, 1.0, 0.0).astype(BF16), table, (((1,), (1,)), ((), ())), preferred_element_type=F32)


def scaled_rows(wide, gain):
    scaled = wide * lax.rsqrt(jnp.mean(wide * wide, axis=-1, keepdims=True) + NORM_EPS)
    return (scaled * gain).astype(BF16)


def head_pair_probs(q_pair, k_head):
    tokens, head_dim = k_head.shape
    scores = lax.dot_general(q_pair, k_head, (((1,), (1,)), ((), ())), preferred_element_type=F32) * head_dim ** -0.5
    row = lax.broadcasted_iota(jnp.int32, (tokens, tokens), 0)
    col = lax.broadcasted_iota(jnp.int32, (tokens, tokens), 1)
    causal = row >= col
    scores = jnp.where(jnp.concatenate([causal, causal], axis=0), scores, -1e30)
    weights = jnp.exp(scores - jnp.max(scores, axis=-1, keepdims=True))
    return weights / jnp.sum(weights, axis=-1, keepdims=True)


def attention_rows(x_ref, gain, wq, wk, wv, wo, head_dim, q_s, k_s, v_s, ctx_s, normed_s):
    tokens = x_ref.shape[0]
    normed_s[...] = scaled_rows(x_ref[...].astype(F32), gain)
    q_s[...] = jnp.dot(normed_s[...], wq[...], preferred_element_type=F32).astype(BF16)
    k_s[...] = jnp.dot(normed_s[...], wk[...], preferred_element_type=F32).astype(BF16)
    v_s[...] = jnp.dot(normed_s[...], wv[...], preferred_element_type=F32).astype(BF16)
    pack = 2 * head_dim

    def pair(m, carry):
        k_two = k_s[:, pl.ds(m * pack, pack)]
        v_two = v_s[:, pl.ds(m * pack, pack)]
        for j in range(2):
            cols = pl.ds((2 * m + j) * pack, pack)
            q_two = q_s[:, cols]
            q_pair = jnp.concatenate([q_two[:, :head_dim], q_two[:, head_dim:]], axis=0)
            k_head = k_two[:, j * head_dim:(j + 1) * head_dim]
            v_head = v_two[:, j * head_dim:(j + 1) * head_dim]
            probs = head_pair_probs(q_pair, k_head).astype(BF16)
            ctx = jnp.dot(probs, v_head, preferred_element_type=F32).astype(BF16)
            ctx_s[:, cols] = jnp.concatenate([ctx[:tokens], ctx[tokens:]], axis=1)
        return carry

    lax.fori_loop(0, k_s.shape[1] // pack, pair, 0)
    return jnp.dot(ctx_s[...], wo[...], preferred_element_type=F32)


NT = (((1,), (1,)), ((), ()))
TN = (((0,), (0,)), ((), ()))


def norm_pull(wide, gain, grad):
    scale = lax.rsqrt(jnp.mean(wide * wide, axis=-1, keepdims=True) + NORM_EPS)
    grad_gain = jnp.sum(grad * (wide * scale), axis=0, keepdims=True)
    lifted = grad * gain
    pull = lifted * scale - wide * (scale * scale * scale * jnp.mean(lifted * wide, axis=-1, keepdims=True))
    return pull.astype(BF16), grad_gain.astype(BF16).astype(F32)


def attention_backward(head_dim, x_ref, dy_ref, du_ref, gains_ref, wq, wk, wv, wo, dx_ref, gq, gk, gv, go, gn, q_s, k_s, v_s, ctx_s, normed_s, dctx_s, dq_s, dk_s, dv_s, dh_s, h_s):
    tokens = x_ref.shape[0]
    gain_1, gain_2 = gains_ref[0:1].astype(F32), gains_ref[1:2].astype(F32)
    pulled, grad_gain = norm_pull(h_s[...].astype(F32), gain_2, du_ref[...].astype(F32))
    gn[1:2, :] = grad_gain
    dh_s[...] = (dy_ref[...].astype(F32) + pulled.astype(F32)).astype(BF16)
    dctx_s[...] = lax.dot_general(dh_s[...], wo[...], NT, preferred_element_type=F32).astype(BF16)
    go[...] = lax.dot_general(ctx_s[...], dh_s[...], TN, preferred_element_type=F32).astype(BF16)
    pack = 2 * head_dim

    def stack(two):
        return jnp.concatenate([two[:, :head_dim], two[:, head_dim:]], axis=0)

    def pair(m, carry):
        tile = pl.ds(m * pack, pack)
        k_two, v_two = k_s[:, tile], v_s[:, tile]
        dk, dv = [], []
        for j in range(2):
            cols = pl.ds((2 * m + j) * pack, pack)
            q_pair, dctx_pair = stack(q_s[:, cols]), stack(dctx_s[:, cols])
            k_head = k_two[:, j * head_dim:(j + 1) * head_dim]
            v_head = v_two[:, j * head_dim:(j + 1) * head_dim]
            probs = head_pair_probs(q_pair, k_head)
            dprobs = lax.dot_general(dctx_pair, v_head, NT, preferred_element_type=F32).astype(BF16).astype(F32)
            dv.append(lax.dot_general(probs.astype(BF16), dctx_pair, TN, preferred_element_type=F32).astype(BF16))
            dscores = probs * (dprobs - jnp.sum(dprobs * probs, axis=-1, keepdims=True))
            dscores = (dscores * head_dim ** -0.5).astype(BF16)
            dq = jnp.dot(dscores, k_head, preferred_element_type=F32).astype(BF16)
            dq_s[:, cols] = jnp.concatenate([dq[:tokens], dq[tokens:]], axis=1)
            dk.append(lax.dot_general(dscores, q_pair, TN, preferred_element_type=F32).astype(BF16))
        dk_s[:, tile] = jnp.concatenate(dk, axis=1)
        dv_s[:, tile] = jnp.concatenate(dv, axis=1)
        return carry

    lax.fori_loop(0, k_s.shape[1] // pack, pair, 0)
    for grad, source in ((gq, dq_s), (gk, dk_s), (gv, dv_s)):
        grad[...] = lax.dot_general(normed_s[...], source[...], TN, preferred_element_type=F32).astype(BF16)
    dnormed = sum(lax.dot_general(source[...], weight[...], NT, preferred_element_type=F32) for source, weight in ((dq_s, wq), (dk_s, wk), (dv_s, wv)))
    pulled, grad_gain = norm_pull(x_ref[...].astype(F32), gain_1, dnormed.astype(BF16).astype(F32))
    gn[0:1, :] = grad_gain
    dx_ref[...] = (dh_s[...].astype(F32) + pulled.astype(F32)).astype(BF16)


BLOCKS = 4


def backward_kernel(side, experts, head_dim, dy_ref, x_ref, eid_a, slot_a, gate_a, eid_b, slot_b, gate_b, ub_ref, w1_ref, w2_ref, w3_ref, gains_ref, wq_ref, wk_ref, wv_ref, wo_ref, u_all, meta_all, du_ref, gw1, gw2, gw3, h_ref, buf, w13, w13t, w2t, tile, dout, acts, dtile, u_ref, loc, tin, tout, sa, ra, sb, rb):
    me, y, x, core = place_of(side)
    partners = [dev(side, y, (x + k) % side, core) for k in range(1, side)]
    partners += [dev(side, (y + k) % side, x, core) for k in range(1, side)]
    partners += [dev(side, y, x, 1 - core)]
    dim = x_ref.shape[-1]
    width = w2_ref.shape[0]
    own_dy = pltpu.make_async_copy(dy_ref, buf.at[y, x, core, :, pl.ds(0, dim)], loc.at[0])
    own_u = pltpu.make_async_copy(u_ref, u_all.at[y, x, core], loc.at[1])
    greet(partners)
    own_dy.start()
    buf[y, x, core, :, dim:] = slot_table((eid_a, slot_a, gate_a, eid_b, slot_b, gate_b), experts)
    first = Gather(side, buf, dim // 2, sa, ra)
    second = Gather(side, u_all, dim // 2 + dim // 8, sb, rb)
    own_dy.wait()
    first.owns()
    start(first.line[0])
    tokens = x_ref.shape[0]
    kv = wk_ref.shape[1]
    attn = attention_rows(x_ref, gains_ref[0:1].astype(F32), wq_ref, wk_ref, wv_ref, wo_ref, head_dim, acts.at[pl.ds(0, tokens)], dout.at[pl.ds(0, tokens), pl.ds(0, kv)], dout.at[pl.ds(0, tokens), pl.ds(kv, kv)], acts.at[pl.ds(tokens, tokens)], dout.at[pl.ds(tokens, tokens)])
    h_ref[...] = (x_ref[...].astype(F32) + attn.astype(BF16).astype(F32)).astype(BF16)
    u_ref[...] = scaled_rows(h_ref[...].astype(F32), gains_ref[1:2].astype(F32))
    own_u.start()
    first.lines()
    w13[:, :width] = w1_ref[...]
    w13[:, width:] = w3_ref[...]
    w13t[...] = w13[...].T
    w2t[...] = w2_ref[...].T
    gw1[...] = jnp.zeros_like(gw1)
    gw2[...] = jnp.zeros_like(gw2)
    gw3[...] = jnp.zeros_like(gw3)
    own_u.wait()
    second.owns()
    first.relays((0, 1, 3, 2))
    start(second.line[0])
    first.rest_of_lines()
    arrive(first.twin_own + first.twin_line)

    slots = du_ref.shape[1]
    group = du_ref.shape[0]
    rows = BLOCKS * slots
    steps = group // BLOCKS

    def turn(g):
        far = jnp.where(g < 3, 0, jnp.where(g < 6, 1, g - 6))
        near = jnp.where(g < 3, g, jnp.where(g < 6, g - 3, 3))
        near = near + jnp.where(near == 2, 1, 0) - jnp.where(near == 3, 1, 0)
        pair = x // 2
        return ((y + near) % side) * (side // 2) + jnp.where(far == 1, 1 - pair, pair)

    def fetch(g, slot):
        return pltpu.make_async_copy(ub_ref.at[pl.ds(turn(g) * rows, rows)], tile.at[slot], tin.at[slot])

    def put(g, slot):
        return pltpu.make_async_copy(dtile.at[slot], du_ref.at[pl.ds(turn(g) * BLOCKS, BLOCKS)], tout.at[slot])

    fetch(0, 0).start()
    spot = lax.broadcasted_iota(jnp.int32, (slots, 1), 0).astype(F32) + 1.0

    def step(g, carry):
        slot = g % 2

        @pl.when(g == 1)
        def _():
            second.lines()

        @pl.when(g == 2)
        def _():
            first.fars()

        @pl.when(g == 3)
        def _():
            arrive(first.twin_far)

        @pl.when(g == 6)
        def _():
            second.relays((0, 1))

        @pl.when(g == 7)
        def _():
            second.relays((3,))
        fetch(g, slot).wait()

        @pl.when(g + 1 < steps)
        def _():
            fetch(g + 1, 1 - slot).start()
        for j in range(BLOCKS):
            p = turn(g) * BLOCKS + j
            block = buf.at[p // (side * CORES), (p // CORES) % side, p % CORES]
            lines = my_rows(block[:, dim:], experts, me, 2 * experts)
            pick = jnp.where(lines[0:1] == spot, lines[1:2], 0.0).astype(BF16)
            dout[pl.ds(j * slots, slots), :] = jnp.dot(pick, block[:, :dim], preferred_element_type=F32).astype(BF16)
        pre = jnp.dot(tile[slot], w13[...], preferred_element_type=F32).astype(BF16).astype(F32)
        pre_1, pre_3 = pre[:, :width], pre[:, width:]
        sigma = jax.nn.sigmoid(pre_1)
        silu_1 = pre_1 * sigma
        hid = (silu_1 * pre_3).astype(BF16)
        grad_hid = jnp.dot(dout[...], w2t[...], preferred_element_type=F32).astype(BF16).astype(F32)
        acts[:, :width] = (grad_hid * pre_3 * sigma * (1.0 + pre_1 * (1.0 - sigma))).astype(BF16)
        acts[:, width:] = (grad_hid * silu_1).astype(BF16)

        @pl.when(g >= 2)
        def _():
            put(g - 2, slot).wait()
        grad_in = jnp.dot(acts[...], w13t[...], preferred_element_type=F32).astype(BF16)
        dtile[slot] = grad_in.reshape(BLOCKS, slots, dim)
        put(g, slot).start()
        over = (((0,), (0,)), ((), ()))
        gw2[...] += lax.dot_general(hid, dout[...], over, preferred_element_type=F32)
        both = lax.dot_general(tile[slot], acts[...], over, preferred_element_type=F32)
        gw1[...] += both[:, :width]
        gw3[...] += both[:, width:]
        return carry

    lax.fori_loop(0, steps, step, 0)
    second.relays((2,))
    second.rest_of_lines()
    second.fars()
    meta_out = pltpu.make_async_copy(buf.at[:, :, :, :, pl.ds(dim, buf.shape[-1] - dim)], meta_all, loc.at[0])
    meta_out.start()
    put(steps - 2, steps % 2).wait()
    put(steps - 1, 1 - steps % 2).wait()
    second.finish()
    first.drain()
    second.drain()
    meta_out.wait()


def run_backward(dy, x_a, routes, saved, weights, head_dim, group):
    side = int(round((group // CORES) ** 0.5))
    rows, dim = x_a.shape
    wide = dim + 4 * group
    slots = saved.shape[0] // group
    width = weights[1].shape[0]
    tall = BLOCKS * slots
    any_spec, vmem = pl.BlockSpec(memory_space=pl.ANY), pl.BlockSpec(memory_space=pltpu.VMEM)
    return pl.pallas_call(
        functools.partial(backward_kernel, side, group, head_dim),
        out_shape=[
            jax.ShapeDtypeStruct((side, side, CORES, rows, dim), BF16),
            jax.ShapeDtypeStruct((side, side, CORES, rows, wide - dim), BF16),
            jax.ShapeDtypeStruct((group, slots, dim), BF16),
            jax.ShapeDtypeStruct((dim, width), F32),
            jax.ShapeDtypeStruct((width, dim), F32),
            jax.ShapeDtypeStruct((dim, width), F32),
            jax.ShapeDtypeStruct((rows, dim), BF16),
        ],
        in_specs=[any_spec, vmem] + [vmem] * len(routes) + [any_spec] + [vmem] * len(weights),
        out_specs=[any_spec, any_spec, any_spec, vmem, vmem, vmem, vmem],
        scratch_shapes=[
            pltpu.VMEM((side, side, CORES, rows, wide), BF16),
            pltpu.VMEM((dim, 2 * width), BF16),
            pltpu.VMEM((2 * width, dim), BF16),
            pltpu.VMEM((dim, width), BF16),
            pltpu.VMEM((2, tall, dim), BF16),
            pltpu.VMEM((tall, dim), BF16),
            pltpu.VMEM((tall, 2 * width), BF16),
            pltpu.VMEM((2, BLOCKS, slots, dim), BF16),
            pltpu.VMEM((rows, dim), BF16),
            pltpu.SemaphoreType.DMA((2,)),
            pltpu.SemaphoreType.DMA((2,)),
            pltpu.SemaphoreType.DMA((2,)),
        ] + [pltpu.SemaphoreType.DMA((GATHER_COPIES,))] * 4,
        compiler_params=pltpu.CompilerParams(collective_id=0, has_side_effects=True, vmem_limit_bytes=64000000),
    )(dy, x_a, *routes, saved, *weights)


class Return:
    def __init__(self, side, experts, offset, gated, slots_ref, meta, bufs, sems):
        self.side, self.experts, self.offset, self.gated, self.src, self.meta = side, experts, offset, gated, slots_ref, meta
        self.r1l, self.r1r, self.ps_l, self.ps_r, self.p2l, self.p2r = bufs
        self.loc, self.s1, self.v1, self.s2, self.v2 = sems
        _, y, x, core = self.spot = place_of(side)
        self.peers = side * CORES
        self.slots, self.half = slots_ref.shape[-2], slots_ref.shape[-1] // 2
        half = self.half
        self.first, self.second_l, self.second_r = [], [], []
        q_row, q_col = x * CORES + core, y * CORES + core
        for i, (k, dc) in enumerate(return_moves(side)):
            xt, yt, ct = (x + k) % side, (y + k) % side, (core + dc) % CORES
            self.first.append(pltpu.make_async_remote_copy(src_ref=slots_ref.at[:, xt, ct, :, pl.ds(0, half)], dst_ref=self.r1l.at[:, q_row], send_sem=self.s1.at[0, i], recv_sem=self.v1.at[0, i], device_id=dev(side, y, xt, ct), device_id_type=MESH_ID))
            self.first.append(pltpu.make_async_remote_copy(src_ref=slots_ref.at[yt, :, ct, :, pl.ds(half, half)], dst_ref=self.r1r.at[:, q_col], send_sem=self.s1.at[1, i], recv_sem=self.v1.at[1, i], device_id=dev(side, yt, x, ct), device_id_type=MESH_ID))
        self.own = [pltpu.make_async_copy(slots_ref.at[:, x, core, :, pl.ds(0, half)], self.r1l.at[:, q_row], self.loc.at[0]),
                    pltpu.make_async_copy(slots_ref.at[y, :, core, :, pl.ds(half, half)], self.r1r.at[:, q_col], self.loc.at[1])]
        for i in range(1, side):
            yt, xt = (y + i) % side, (x + i) % side
            self.second_l.append(pltpu.make_async_remote_copy(src_ref=self.ps_l.at[yt], dst_ref=self.p2l.at[i - 1], send_sem=self.s2.at[0, i], recv_sem=self.v2.at[0, i], device_id=dev(side, yt, x, core), device_id_type=MESH_ID))
            self.second_r.append(pltpu.make_async_remote_copy(src_ref=self.ps_r.at[xt], dst_ref=self.p2r.at[i - 1], send_sem=self.s2.at[1, i], recv_sem=self.v2.at[1, i], device_id=dev(side, y, xt, core), device_id_type=MESH_ID))

    def launch(self):
        start(self.first)
        start(self.own)

    def selector(self, ids):
        wide = self.meta.shape[-1]
        src = lax.broadcasted_iota(jnp.int32, (wide, wide), 0)
        dst = lax.broadcasted_iota(jnp.int32, (wide, wide), 1)
        hit = jnp.zeros((wide, wide), F32)
        for q, e in enumerate(ids):
            hit = jnp.where((src == self.offset + e) & (dst == q), 1.0, hit)
            hit = jnp.where((src == self.offset + self.experts + e) & (dst == self.peers + q), 1.0, hit)
        return hit.astype(BF16)

    def partial(self, block, sel, landed, sums, k):
        lane = lax.broadcasted_iota(jnp.int32, (1, self.slots), 1).astype(F32) + 1.0
        table = jnp.dot(block, sel, preferred_element_type=F32)
        weights = []
        for q in range(self.peers):
            scale = table[:, self.peers + q:self.peers + q + 1] if self.gated else 1.0
            weights.append(jnp.where(table[:, q:q + 1] == lane, scale, 0.0).astype(BF16))
        vals = landed[k].reshape(self.peers * self.slots, self.half)
        sums[k] = jnp.dot(jnp.concatenate(weights, axis=1), vals, preferred_element_type=F32)

    def sum_and_send(self):
        _, y, x, core = self.spot
        side = self.side
        for copy in self.own:
            copy.wait()
        arrive(self.first)
        sel_l = self.selector([y * self.peers + q for q in range(self.peers)])
        sel_r = self.selector([((q // CORES) * side + x) * CORES + q % CORES for q in range(self.peers)])
        for i in range(1, side + 1):
            ky, kx = (y + i) % side, (x + i) % side
            self.partial(self.meta[ky, x, core], sel_l, self.r1l, self.ps_l, ky)
            if i > 1:
                self.second_r[i - 2].start()
            self.partial(self.meta[y, kx, core], sel_r, self.r1r, self.ps_r, kx)
            if i < side:
                self.second_l[i - 1].start()

    def total(self, base, out_ref):
        _, y, x, core = self.spot
        half = self.half
        arrive(self.second_l + self.second_r)
        for cols, sums, k, landed in ((slice(0, half), self.ps_l, y, self.p2l), (slice(half, 2 * half), self.ps_r, x, self.p2r)):
            total = sums[k] if base is None else base[:, cols].astype(F32) + sums[k]
            for i in range(1, self.side):
                total = total + landed[i - 1]
            out_ref[:, cols] = total.astype(BF16)

    def drain(self):
        sent(self.first + self.second_l + self.second_r)


def return_moves(side):
    return [(k, dc) for k in range(1, side) for dc in range(CORES)] + [(0, 1)]


RETURN_BUFFERS = 6


def return_kernel(side, experts, head_dim, slots_b, u_all, meta_ref, w1_ref, w2_ref, w3_ref, h_ref, x_ref, dy_ref, gains_ref, wq, wk, wv, wo, y_ref, dx_ref, gq, gk, gv, go, gn, fwd_ref, meta, w13, w2, utile, recv, otile, du_s, *rest):
    bufs_b, bufs_a, rest = rest[:RETURN_BUFFERS], rest[RETURN_BUFFERS:2 * RETURN_BUFFERS], rest[2 * RETURN_BUFFERS:]
    att, rest = rest[:11], rest[11:]
    sems_b, sems_a, (loc, tin, tout) = rest[:5], rest[5:10], rest[10:]
    me, y, x, core = place_of(side)
    partners = [(y, (x + k) % side, (core + dc) % CORES) for k, dc in return_moves(side)]
    partners += [((y + k) % side, x, (core + dc) % CORES) for k, dc in return_moves(side) if k]
    greet([dev(side, *spot) for spot in partners])
    back_b = Return(side, experts, 2 * experts, False, slots_b, meta, bufs_b, sems_b)
    back_a = Return(side, experts, 0, True, fwd_ref, meta, bufs_a, sems_a)
    back_b.launch()
    width = w2_ref.shape[0]
    slots = fwd_ref.shape[3]
    dim = x_ref.shape[-1]
    loads = [pltpu.make_async_copy(meta_ref, meta, loc.at[0]), pltpu.make_async_copy(w2_ref, w2, loc.at[1]),
             pltpu.make_async_copy(w1_ref, w13.at[:, pl.ds(0, width)], loc.at[2]), pltpu.make_async_copy(w3_ref, w13.at[:, pl.ds(width, width)], loc.at[3])]
    start(loads)
    steps = side * side
    spot = lax.broadcasted_iota(jnp.int32, (slots, 1), 0).astype(F32) + 1.0

    def fetch(g, slot):
        return pltpu.make_async_copy(u_all.at[g // side, g % side], utile.at[slot], tin.at[slot])

    def put(g, slot):
        return pltpu.make_async_copy(otile.at[slot], fwd_ref.at[g // side, g % side], tout.at[slot])

    fetch(0, 0).start()
    for copy in loads:
        copy.wait()

    def step(g, carry):
        slot = g % 2
        fetch(g, slot).wait()

        @pl.when(g + 1 < steps)
        def _():
            fetch(g + 1, 1 - slot).start()
        for j in range(CORES):
            lines = my_rows(meta[g // side, g % side, j], experts, me, 0)
            pick = jnp.where(lines[0:1] == spot, 1.0, 0.0).astype(BF16)
            recv[pl.ds(j * slots, slots), :] = jnp.dot(pick, utile[slot, j], preferred_element_type=F32).astype(BF16)
        act = jnp.dot(recv[...], w13[...], preferred_element_type=F32).astype(BF16).astype(F32)
        act_1, act_3 = act[:, :width], act[:, width:]
        hidden = (act_1 * jax.nn.sigmoid(act_1) * act_3).astype(BF16)

        @pl.when(g >= 2)
        def _():
            put(g - 2, slot).wait()
        otile[slot] = jnp.dot(hidden, w2[...], preferred_element_type=F32).astype(BF16).reshape(CORES, slots, dim)
        put(g, slot).start()
        return carry

    lax.fori_loop(0, steps, step, 0)
    put(steps - 2, steps % 2).wait()
    put(steps - 1, 1 - steps % 2).wait()
    back_a.launch()
    q_s, k_s, v_s, ctx_s, normed_s = att[:5]
    attn = attention_rows(x_ref, gains_ref[0:1].astype(F32), wq, wk, wv, wo, head_dim, q_s, k_s, v_s, ctx_s, normed_s)
    att[10][...] = (x_ref[...].astype(F32) + attn.astype(BF16).astype(F32)).astype(BF16)
    back_b.sum_and_send()
    back_a.sum_and_send()
    back_b.total(None, du_s)
    attention_backward(head_dim, x_ref, dy_ref, du_s, gains_ref, wq, wk, wv, wo, dx_ref, gq, gk, gv, go, gn, *att)
    back_a.total(h_ref, y_ref)
    back_b.drain()
    back_a.drain()


def run_returns(slots_b, u_all, meta, experts_w, h_a, x_b, dy_b, gains, flat, head_dim, group):
    side = meta.shape[0]
    capacity, dim = slots_b.shape[1:]
    rows = x_b.shape[0]
    half = dim // 2
    peers = side * CORES
    width = experts_w[1].shape[0]
    full, kv = flat[0].shape[1], flat[1].shape[1]
    any_spec, vmem = pl.BlockSpec(memory_space=pl.ANY), pl.BlockSpec(memory_space=pltpu.VMEM)
    cube = slots_b.reshape(side, side, CORES, capacity, dim)
    sets = [pltpu.VMEM((side, peers, capacity, half), BF16)] * 2 + [pltpu.VMEM((side, rows, half), F32)] * 2 + [pltpu.VMEM((side - 1, rows, half), F32)] * 2
    sems = [pltpu.SemaphoreType.DMA((2,)), pltpu.SemaphoreType.DMA((2, peers)), pltpu.SemaphoreType.DMA((2, peers)), pltpu.SemaphoreType.DMA((2, side)), pltpu.SemaphoreType.DMA((2, side))]
    return pl.pallas_call(
        functools.partial(return_kernel, side, group, head_dim),
        out_shape=[jax.ShapeDtypeStruct(x_b.shape, BF16)] * 2 + [jax.ShapeDtypeStruct(part.shape, BF16) for part in flat] + [jax.ShapeDtypeStruct((2, dim), F32), jax.ShapeDtypeStruct(cube.shape, BF16)],
        in_specs=[any_spec] * 6 + [vmem] * 8,
        out_specs=[vmem] * 7 + [any_spec],
        scratch_shapes=[
            pltpu.VMEM(meta.shape, BF16),
            pltpu.VMEM((dim, 2 * width), BF16),
            pltpu.VMEM((width, dim), BF16),
            pltpu.VMEM((2, CORES, rows, dim), BF16),
            pltpu.VMEM((CORES * capacity, dim), BF16),
            pltpu.VMEM((2, CORES, capacity, dim), BF16),
            pltpu.VMEM((rows, dim), BF16),
        ] + sets + sets + [pltpu.VMEM((rows, cols), BF16) for cols in (full, kv, kv, full, dim, full, full, kv, kv, dim, dim)] + sems + sems + [pltpu.SemaphoreType.DMA((4,)), pltpu.SemaphoreType.DMA((2,)), pltpu.SemaphoreType.DMA((2,))],
        compiler_params=pltpu.CompilerParams(collective_id=1, has_side_effects=True, vmem_limit_bytes=67043328),
    )(cube, u_all, meta, *experts_w, h_a, x_b, dy_b, gains, *flat)


def solution(mesh):
    group = mesh.shape['expert']

    def local_step(x_a, x_b, dy_b, eid_a, slot_a, gate_a, eid_b, slot_b, gate_b, u_b, norm_1, norm_2, w_q, w_k, w_v, w_o, w_1, w_2, w_3):
        rows, model_dim = x_a.shape
        w1, w2, w3 = w_1[0], w_2[0], w_3[0]

        head_dim = w_q.shape[2]
        gains = jnp.stack([norm_1, norm_2])
        routes = tuple(part.T for part in (eid_a, slot_a, gate_a, eid_b, slot_b, gate_b))
        flat = (w_q.reshape(model_dim, -1), w_k.reshape(model_dim, -1), w_v.reshape(model_dim, -1), w_o.reshape(-1, model_dim))

        u_all, meta, grad_in, grad_w1, grad_w2, grad_w3, h_a = run_backward(dy_b, x_a, routes, u_b[0], (w1, w2, w3, gains) + flat, head_dim, group)
        y_a, dx_b, g_q, g_k, g_v, g_o, g_n, _ = run_returns(grad_in, u_all, meta, (w1, w2, w3), h_a, x_b, dy_b, gains, flat, head_dim, group)
        grads = tuple(g.reshape(w.shape).astype(F32)[None] for g, w in ((g_q, w_q), (g_k, w_k), (g_v, w_v), (g_o, w_o))) + (g_n[0:1], g_n[1:2])
        return (y_a, dx_b, grad_w1[None], grad_w2[None], grad_w3[None], *grads)

    row_spec = P(('data', 'expert'), None)
    cube_spec = P(('data', 'expert'), None, None)
    quad_spec = P(('data', 'expert'), None, None, None)
    expert_spec = P('expert', None, None)
    in_specs = (row_spec, row_spec, row_spec, row_spec, row_spec, row_spec, row_spec, row_spec, row_spec, cube_spec, P(), P(), P(), P(), P(), P(), expert_spec, expert_spec, expert_spec)
    out_specs = (row_spec, row_spec, cube_spec, cube_spec, cube_spec, quad_spec, quad_spec, quad_spec, quad_spec, row_spec, row_spec)
    return jax.shard_map(local_step, mesh=mesh, in_specs=in_specs, out_specs=out_specs, check_vma=False)
```

```python
import functools

import jax
import jax.numpy as jnp
from jax import lax
from jax.experimental import pallas as pl
from jax.experimental.pallas import tpu as pltpu
from jax.sharding import PartitionSpec as P

NORM_EPS = 1e-6
CORES = 2
BF16 = jnp.bfloat16
F32 = jnp.float32
MESH_ID = pl.DeviceIdType.MESH


def slot_table(routes, experts):
    choices, rows = routes[0].shape
    columns = [part[...].astype(F32).T for part in routes]
    lane = lax.broadcasted_iota(jnp.int32, (rows, 4 * experts), 1).astype(F32)
    table = jnp.zeros(lane.shape, F32)
    for i in range(2):
        for j in range(choices):
            eid, slot, gate = [columns[3 * i + k][:, j:j + 1] for k in range(3)]
            spot = eid + 2.0 * i * experts
            table = jnp.where(lane == spot, slot + 1.0, table)
            table = jnp.where(lane == spot + experts, gate, table)
    return table.astype(BF16)


def place_of(side_x):
    me = lax.axis_index('expert')
    core = me % CORES
    return me, me // (CORES * side_x), (me // CORES) % side_x, core


def dev(side_x, yy, xx, cc):
    return {'expert': (yy * side_x + xx) * CORES + cc}


def greet(partners):
    barrier = pltpu.get_barrier_semaphore()
    for spot in partners:
        pl.semaphore_signal(barrier, inc=1, device_id=spot, device_id_type=MESH_ID)
    pl.semaphore_wait(barrier, len(partners))


class Gather:
    def __init__(self, side, buf, cut, send, recv):
        self.side, self.buf, self.send, self.recv = side, buf, send, recv
        _, self.y, self.x, self.core = place_of(side)
        width = buf.shape[-1]
        self.left, self.right = pl.ds(0, cut), pl.ds(cut, width - cut)
        self.count = 0
        y, x, c, side = self.y, self.x, self.core, self.side
        up, down, far = (y + 1) % side, (y + side - 1) % side, (y + 2) % side
        east, west, over = (x + 1) % side, (x + side - 1) % side, (x + 2) % side
        every = pl.ds(0, side)
        twin = 1 - c
        L, R = self.left, self.right
        self.own, self.line, self.relay = [], [], []
        for k in range(1, side):
            self.own.append([self.make((y, x, c, L), (y, (x + k) % side, c)), self.make((y, x, c, R), ((y + k) % side, x, c))])
        for k in range(side):
            xx, yy = (x + side - k) % side, (y + side - k) % side
            self.line.append([self.make((y, xx, c, L), (up, x, c)), self.make((yy, x, c, R), (y, east, c)),
                              self.make((y, xx, c, L), (down, x, c)), self.make((yy, x, c, R), (y, west, c))])
        for k in range(side):
            xx, yy = (x + side - k) % side, (y + side - k) % side
            if k < 2:
                self.relay.append([self.make((down, xx, c, L), (up, x, c)), self.make((yy, west, c, R), (y, east, c))])
            else:
                self.relay.append([self.make((up, xx, c, L), (down, x, c)), self.make((yy, east, c, R), (y, west, c))])
        self.twin_own = [self.make((y, every, c, L), (y, x, twin)), self.make((every, x, c, R), (y, x, twin))]
        self.twin_line = [self.make((up, every, c, L), (y, x, twin)), self.make((every, east, c, R), (y, x, twin)),
                          self.make((down, every, c, L), (y, x, twin)), self.make((every, west, c, R), (y, x, twin))]
        self.twin_far = [self.make((far, every, c, L), (y, x, twin)), self.make((every, over, c, R), (y, x, twin))]

    def owns(self):
        for k in (0, 2, 1):
            start(self.own[k])

    def lines(self):
        for k in (1, 3, 2):
            arrive(self.own[k - 1])
            start(self.line[k])
        start(self.twin_own)

    def relays(self, order):
        for k in order:
            arrive(self.line[k][:2] if k < 2 else self.line[k][2:])
            start(self.relay[k])

    def rest_of_lines(self):
        for k in (2, 3):
            arrive(self.line[k][:2])
        for k in (0, 1):
            arrive(self.line[k][2:])
        start(self.twin_line)

    def fars(self):
        for k in range(self.side):
            arrive(self.relay[k])
        start(self.twin_far)

    def finish(self):
        arrive(self.twin_own + self.twin_line + self.twin_far)

    def drain(self):
        sent(sum(self.own + self.line + self.relay, []) + self.twin_own + self.twin_line + self.twin_far)

    def make(self, spot, target):
        yy, xx, cc, cols = spot
        part = self.buf.at[yy, xx, cc, :, cols]
        i = self.count
        self.count += 1
        return pltpu.make_async_remote_copy(src_ref=part, dst_ref=part, send_sem=self.send.at[i], recv_sem=self.recv.at[i], device_id=dev(self.side, *target), device_id_type=MESH_ID)


GATHER_COPIES = 38


def start(copies):
    for copy in copies:
        copy.start()


def arrive(copies):
    for copy in copies:
        copy.wait_recv()


def sent(copies):
    for copy in copies:
        copy.wait_send()


def my_rows(table, experts, me, offset):
    row = lax.broadcasted_iota(jnp.int32, (8, table.shape[-1]), 0)
    lane = lax.broadcasted_iota(jnp.int32, (8, table.shape[-1]), 1)
    pick = ((lane == offset + me) & (row == 0)) | ((lane == offset + experts + me) & (row == 1))
    return lax.dot_general(jnp.where(pick, 1.0, 0.0).astype(BF16), table, (((1,), (1,)), ((), ())), preferred_element_type=F32)


def scaled_rows(wide, gain):
    scaled = wide * lax.rsqrt(jnp.mean(wide * wide, axis=-1, keepdims=True) + NORM_EPS)
    return (scaled * gain).astype(BF16)


def head_pair_probs(q_pair, k_head):
    tokens, head_dim = k_head.shape
    scores = lax.dot_general(q_pair, k_head, (((1,), (1,)), ((), ())), preferred_element_type=F32) * head_dim ** -0.5
    row = lax.broadcasted_iota(jnp.int32, (tokens, tokens), 0)
    col = lax.broadcasted_iota(jnp.int32, (tokens, tokens), 1)
    causal = row >= col
    scores = jnp.where(jnp.concatenate([causal, causal], axis=0), scores, -1e30)
    weights = jnp.exp(scores - jnp.max(scores, axis=-1, keepdims=True))
    return weights / jnp.sum(weights, axis=-1, keepdims=True)


def attention_rows(x_ref, gain, wq, wk, wv, wo, head_dim, q_s, k_s, v_s, ctx_s, normed_s):
    tokens = x_ref.shape[0]
    normed_s[...] = scaled_rows(x_ref[...].astype(F32), gain)
    q_s[...] = jnp.dot(normed_s[...], wq[...], preferred_element_type=F32).astype(BF16)
    k_s[...] = jnp.dot(normed_s[...], wk[...], preferred_element_type=F32).astype(BF16)
    v_s[...] = jnp.dot(normed_s[...], wv[...], preferred_element_type=F32).astype(BF16)
    pack = 2 * head_dim

    def pair(m, carry):
        k_two = k_s[:, pl.ds(m * pack, pack)]
        v_two = v_s[:, pl.ds(m * pack, pack)]
        for j in range(2):
            cols = pl.ds((2 * m + j) * pack, pack)
            q_two = q_s[:, cols]
            q_pair = jnp.concatenate([q_two[:, :head_dim], q_two[:, head_dim:]], axis=0)
            k_head = k_two[:, j * head_dim:(j + 1) * head_dim]
            v_head = v_two[:, j * head_dim:(j + 1) * head_dim]
            probs = head_pair_probs(q_pair, k_head).astype(BF16)
            ctx = jnp.dot(probs, v_head, preferred_element_type=F32).astype(BF16)
            ctx_s[:, cols] = jnp.concatenate([ctx[:tokens], ctx[tokens:]], axis=1)
        return carry

    lax.fori_loop(0, k_s.shape[1] // pack, pair, 0)
    return jnp.dot(ctx_s[...], wo[...], preferred_element_type=F32)


NT = (((1,), (1,)), ((), ()))
TN = (((0,), (0,)), ((), ()))


def norm_pull(wide, gain, grad):
    scale = lax.rsqrt(jnp.mean(wide * wide, axis=-1, keepdims=True) + NORM_EPS)
    grad_gain = jnp.sum(grad * (wide * scale), axis=0, keepdims=True)
    lifted = grad * gain
    pull = lifted * scale - wide * (scale * scale * scale * jnp.mean(lifted * wide, axis=-1, keepdims=True))
    return pull.astype(BF16), grad_gain.astype(BF16).astype(F32)


def attention_backward(head_dim, x_ref, dy_ref, du_ref, gains_ref, wq, wk, wv, wo, dx_ref, gq, gk, gv, go, gn, q_s, k_s, v_s, ctx_s, normed_s, dctx_s, dq_s, dk_s, dv_s, dh_s, h_s):
    tokens = x_ref.shape[0]
    gain_1, gain_2 = gains_ref[0:1].astype(F32), gains_ref[1:2].astype(F32)
    pulled, grad_gain = norm_pull(h_s[...].astype(F32), gain_2, du_ref[...].astype(F32))
    gn[1:2, :] = grad_gain
    dh_s[...] = (dy_ref[...].astype(F32) + pulled.astype(F32)).astype(BF16)
    dctx_s[...] = lax.dot_general(dh_s[...], wo[...], NT, preferred_element_type=F32).astype(BF16)
    go[...] = lax.dot_general(ctx_s[...], dh_s[...], TN, preferred_element_type=F32).astype(BF16)
    pack = 2 * head_dim

    def stack(two):
        return jnp.concatenate([two[:, :head_dim], two[:, head_dim:]], axis=0)

    def pair(m, carry):
        tile = pl.ds(m * pack, pack)
        k_two, v_two = k_s[:, tile], v_s[:, tile]
        dk, dv = [], []
        for j in range(2):
            cols = pl.ds((2 * m + j) * pack, pack)
            q_pair, dctx_pair = stack(q_s[:, cols]), stack(dctx_s[:, cols])
            k_head = k_two[:, j * head_dim:(j + 1) * head_dim]
            v_head = v_two[:, j * head_dim:(j + 1) * head_dim]
            probs = head_pair_probs(q_pair, k_head)
            dprobs = lax.dot_general(dctx_pair, v_head, NT, preferred_element_type=F32).astype(BF16).astype(F32)
            dv.append(lax.dot_general(probs.astype(BF16), dctx_pair, TN, preferred_element_type=F32).astype(BF16))
            dscores = probs * (dprobs - jnp.sum(dprobs * probs, axis=-1, keepdims=True))
            dscores = (dscores * head_dim ** -0.5).astype(BF16)
            dq = jnp.dot(dscores, k_head, preferred_element_type=F32).astype(BF16)
            dq_s[:, cols] = jnp.concatenate([dq[:tokens], dq[tokens:]], axis=1)
            dk.append(lax.dot_general(dscores, q_pair, TN, preferred_element_type=F32).astype(BF16))
        dk_s[:, tile] = jnp.concatenate(dk, axis=1)
        dv_s[:, tile] = jnp.concatenate(dv, axis=1)
        return carry

    lax.fori_loop(0, k_s.shape[1] // pack, pair, 0)
    for grad, source in ((gq, dq_s), (gk, dk_s), (gv, dv_s)):
        grad[...] = lax.dot_general(normed_s[...], source[...], TN, preferred_element_type=F32).astype(BF16)
    dnormed = sum(lax.dot_general(source[...], weight[...], NT, preferred_element_type=F32) for source, weight in ((dq_s, wq), (dk_s, wk), (dv_s, wv)))
    pulled, grad_gain = norm_pull(x_ref[...].astype(F32), gain_1, dnormed.astype(BF16).astype(F32))
    gn[0:1, :] = grad_gain
    dx_ref[...] = (dh_s[...].astype(F32) + pulled.astype(F32)).astype(BF16)


BLOCKS = 4


def backward_kernel(side, experts, head_dim, dy_ref, x_ref, eid_a, slot_a, gate_a, eid_b, slot_b, gate_b, ub_ref, w1_ref, w2_ref, w3_ref, gains_ref, wq_ref, wk_ref, wv_ref, wo_ref, u_all, meta_all, du_ref, gw1, gw2, gw3, h_ref, buf, w13, w13t, w2t, tile, pre_s, dout, acts, dtile, u_ref, loc, tin, tout, sa, ra, sb, rb):
    me, y, x, core = place_of(side)
    partners = [dev(side, y, (x + k) % side, core) for k in range(1, side)]
    partners += [dev(side, (y + k) % side, x, core) for k in range(1, side)]
    partners += [dev(side, y, x, 1 - core)]
    dim = x_ref.shape[-1]
    width = w2_ref.shape[0]
    own_dy = pltpu.make_async_copy(dy_ref, buf.at[y, x, core, :, pl.ds(0, dim)], loc.at[0])
    own_u = pltpu.make_async_copy(u_ref, u_all.at[y, x, core], loc.at[1])
    greet(partners)
    own_dy.start()
    buf[y, x, core, :, dim:] = slot_table((eid_a, slot_a, gate_a, eid_b, slot_b, gate_b), experts)
    first = Gather(side, buf, dim // 2, sa, ra)
    second = Gather(side, u_all, dim // 2 + dim // 8, sb, rb)
    own_dy.wait()
    first.owns()
    start(first.line[0])
    tokens = x_ref.shape[0]
    kv = wk_ref.shape[1]
    attn = attention_rows(x_ref, gains_ref[0:1].astype(F32), wq_ref, wk_ref, wv_ref, wo_ref, head_dim, acts.at[pl.ds(0, tokens)], dout.at[pl.ds(0, tokens), pl.ds(0, kv)], dout.at[pl.ds(0, tokens), pl.ds(kv, kv)], acts.at[pl.ds(tokens, tokens)], dout.at[pl.ds(tokens, tokens)])
    h_ref[...] = (x_ref[...].astype(F32) + attn.astype(BF16).astype(F32)).astype(BF16)
    u_ref[...] = scaled_rows(h_ref[...].astype(F32), gains_ref[1:2].astype(F32))
    own_u.start()
    first.lines()
    w13[:, :width] = w1_ref[...]
    w13[:, width:] = w3_ref[...]
    w13t[...] = w13[...].T
    w2t[...] = w2_ref[...].T
    gw1[...] = jnp.zeros_like(gw1)
    gw2[...] = jnp.zeros_like(gw2)
    gw3[...] = jnp.zeros_like(gw3)
    slots = du_ref.shape[1]
    group = du_ref.shape[0]
    rows = BLOCKS * slots
    steps = group // BLOCKS

    def turn(g):
        far = jnp.where(g < 3, 0, jnp.where(g < 6, 1, g - 6))
        near = jnp.where(g < 3, g, jnp.where(g < 6, g - 3, 3))
        near = near + jnp.where(near == 2, 1, 0) - jnp.where(near == 3, 1, 0)
        pair = x // 2
        return ((y + near) % side) * (side // 2) + jnp.where(far == 1, 1 - pair, pair)

    def fetch(g, slot):
        return pltpu.make_async_copy(ub_ref.at[pl.ds(turn(g) * rows, rows)], tile.at[slot], tin.at[slot])

    def put(g, slot):
        return pltpu.make_async_copy(dtile.at[slot], du_ref.at[pl.ds(turn(g) * BLOCKS, BLOCKS)], tout.at[slot])

    spot = lax.broadcasted_iota(jnp.int32, (slots, 1), 0).astype(F32) + 1.0

    def warm(g, carry):
        slot = g % 2

        @pl.when(g == 4)
        def _():
            first.relays((0, 1))
        fetch(g, slot).wait()

        @pl.when(g + 1 < steps)
        def _():
            fetch(g + 1, 1 - slot).start()
        pre_s[pl.ds(g * rows, rows), :] = jnp.dot(tile[slot], w13[...], preferred_element_type=F32).astype(BF16)
        return carry

    fetch(0, 0).start()
    own_u.wait()
    lax.fori_loop(0, steps, warm, 0)
    fetch(0, 0).start()
    first.relays((3, 2))
    second.owns()
    start(second.line[0])
    first.rest_of_lines()
    arrive(first.twin_own + first.twin_line)

    def step(g, carry):
        slot = g % 2

        @pl.when(g == 3)
        def _():
            second.lines()

        @pl.when(g == 1)
        def _():
            first.fars()

        @pl.when(g == 3)
        def _():
            arrive(first.twin_far)

        @pl.when(g == 6)
        def _():
            second.relays((0, 1))

        @pl.when(g == 7)
        def _():
            second.relays((3,))
        fetch(g, slot).wait()

        @pl.when(g + 1 < steps)
        def _():
            fetch(g + 1, 1 - slot).start()
        for j in range(BLOCKS):
            p = turn(g) * BLOCKS + j
            block = buf.at[p // (side * CORES), (p // CORES) % side, p % CORES]
            lines = my_rows(block[:, dim:], experts, me, 2 * experts)
            pick = jnp.where(lines[0:1] == spot, lines[1:2], 0.0).astype(BF16)
            dout[pl.ds(j * slots, slots), :] = jnp.dot(pick, block[:, :dim], preferred_element_type=F32).astype(BF16)
        pre = pre_s[pl.ds(g * rows, rows), :].astype(F32)
        pre_1, pre_3 = pre[:, :width], pre[:, width:]
        sigma = jax.nn.sigmoid(pre_1)
        silu_1 = pre_1 * sigma
        hid = (silu_1 * pre_3).astype(BF16)
        grad_hid = jnp.dot(dout[...], w2t[...], preferred_element_type=F32).astype(BF16).astype(F32)
        acts[:, :width] = (grad_hid * pre_3 * sigma * (1.0 + pre_1 * (1.0 - sigma))).astype(BF16)
        acts[:, width:] = (grad_hid * silu_1).astype(BF16)

        @pl.when(g >= 2)
        def _():
            put(g - 2, slot).wait()
        grad_in = jnp.dot(acts[...], w13t[...], preferred_element_type=F32).astype(BF16)
        dtile[slot] = grad_in.reshape(BLOCKS, slots, dim)
        put(g, slot).start()
        over = (((0,), (0,)), ((), ()))
        gw2[...] += lax.dot_general(hid, dout[...], over, preferred_element_type=F32)
        both = lax.dot_general(tile[slot], acts[...], over, preferred_element_type=F32)
        gw1[...] += both[:, :width]
        gw3[...] += both[:, width:]
        return carry

    lax.fori_loop(0, steps, step, 0)
    second.relays((2,))
    second.rest_of_lines()
    second.fars()
    meta_out = pltpu.make_async_copy(buf.at[:, :, :, :, pl.ds(dim, buf.shape[-1] - dim)], meta_all, loc.at[0])
    meta_out.start()
    put(steps - 2, steps % 2).wait()
    put(steps - 1, 1 - steps % 2).wait()
    second.finish()
    first.drain()
    second.drain()
    meta_out.wait()


def run_backward(dy, x_a, routes, saved, weights, head_dim, group):
    side = int(round((group // CORES) ** 0.5))
    rows, dim = x_a.shape
    wide = dim + 4 * group
    slots = saved.shape[0] // group
    width = weights[1].shape[0]
    tall = BLOCKS * slots
    any_spec, vmem = pl.BlockSpec(memory_space=pl.ANY), pl.BlockSpec(memory_space=pltpu.VMEM)
    return pl.pallas_call(
        functools.partial(backward_kernel, side, group, head_dim),
        out_shape=[
            jax.ShapeDtypeStruct((side, side, CORES, rows, dim), BF16),
            jax.ShapeDtypeStruct((side, side, CORES, rows, wide - dim), BF16),
            jax.ShapeDtypeStruct((group, slots, dim), BF16),
            jax.ShapeDtypeStruct((dim, width), F32),
            jax.ShapeDtypeStruct((width, dim), F32),
            jax.ShapeDtypeStruct((dim, width), F32),
            jax.ShapeDtypeStruct((rows, dim), BF16),
        ],
        in_specs=[any_spec, vmem] + [vmem] * len(routes) + [any_spec] + [vmem] * len(weights),
        out_specs=[any_spec, any_spec, any_spec, vmem, vmem, vmem, vmem],
        scratch_shapes=[
            pltpu.VMEM((side, side, CORES, rows, wide), BF16),
            pltpu.VMEM((dim, 2 * width), BF16),
            pltpu.VMEM((2 * width, dim), BF16),
            pltpu.VMEM((dim, width), BF16),
            pltpu.VMEM((2, tall, dim), BF16),
            pltpu.VMEM((group * slots, 2 * width), BF16),
            pltpu.VMEM((tall, dim), BF16),
            pltpu.VMEM((tall, 2 * width), BF16),
            pltpu.VMEM((2, BLOCKS, slots, dim), BF16),
            pltpu.VMEM((rows, dim), BF16),
            pltpu.SemaphoreType.DMA((2,)),
            pltpu.SemaphoreType.DMA((2,)),
            pltpu.SemaphoreType.DMA((2,)),
        ] + [pltpu.SemaphoreType.DMA((GATHER_COPIES,))] * 4,
        compiler_params=pltpu.CompilerParams(collective_id=0, has_side_effects=True, vmem_limit_bytes=67043328),
    )(dy, x_a, *routes, saved, *weights)


class Return:
    def __init__(self, side, experts, offset, gated, slots_ref, meta, bufs, sems):
        self.side, self.experts, self.offset, self.gated, self.src, self.meta = side, experts, offset, gated, slots_ref, meta
        self.r1l, self.r1r, self.ps_l, self.ps_r, self.p2l, self.p2r = bufs
        self.loc, self.s1, self.v1, self.s2, self.v2 = sems
        _, y, x, core = self.spot = place_of(side)
        self.peers = side * CORES
        self.slots, self.half = slots_ref.shape[-2], slots_ref.shape[-1] // 2
        half = self.half
        self.first, self.second_l, self.second_r = [], [], []
        q_row, q_col = x * CORES + core, y * CORES + core
        for i, (k, dc) in enumerate(return_moves(side)):
            xt, yt, ct = (x + k) % side, (y + k) % side, (core + dc) % CORES
            self.first.append(pltpu.make_async_remote_copy(src_ref=slots_ref.at[:, xt, ct, :, pl.ds(0, half)], dst_ref=self.r1l.at[:, q_row], send_sem=self.s1.at[0, i], recv_sem=self.v1.at[0, i], device_id=dev(side, y, xt, ct), device_id_type=MESH_ID))
            self.first.append(pltpu.make_async_remote_copy(src_ref=slots_ref.at[yt, :, ct, :, pl.ds(half, half)], dst_ref=self.r1r.at[:, q_col], send_sem=self.s1.at[1, i], recv_sem=self.v1.at[1, i], device_id=dev(side, yt, x, ct), device_id_type=MESH_ID))
        self.own = [pltpu.make_async_copy(slots_ref.at[:, x, core, :, pl.ds(0, half)], self.r1l.at[:, q_row], self.loc.at[0]),
                    pltpu.make_async_copy(slots_ref.at[y, :, core, :, pl.ds(half, half)], self.r1r.at[:, q_col], self.loc.at[1])]
        for i in range(1, side):
            yt, xt = (y + i) % side, (x + i) % side
            self.second_l.append(pltpu.make_async_remote_copy(src_ref=self.ps_l.at[yt], dst_ref=self.p2l.at[i - 1], send_sem=self.s2.at[0, i], recv_sem=self.v2.at[0, i], device_id=dev(side, yt, x, core), device_id_type=MESH_ID))
            self.second_r.append(pltpu.make_async_remote_copy(src_ref=self.ps_r.at[xt], dst_ref=self.p2r.at[i - 1], send_sem=self.s2.at[1, i], recv_sem=self.v2.at[1, i], device_id=dev(side, y, xt, core), device_id_type=MESH_ID))

    def launch(self):
        start(self.first)
        start(self.own)

    def selector(self, ids):
        wide = self.meta.shape[-1]
        src = lax.broadcasted_iota(jnp.int32, (wide, wide), 0)
        dst = lax.broadcasted_iota(jnp.int32, (wide, wide), 1)
        hit = jnp.zeros((wide, wide), F32)
        for q, e in enumerate(ids):
            hit = jnp.where((src == self.offset + e) & (dst == q), 1.0, hit)
            hit = jnp.where((src == self.offset + self.experts + e) & (dst == self.peers + q), 1.0, hit)
        return hit.astype(BF16)

    def partial(self, block, sel, landed, sums, k):
        lane = lax.broadcasted_iota(jnp.int32, (1, self.slots), 1).astype(F32) + 1.0
        table = jnp.dot(block, sel, preferred_element_type=F32)
        weights = []
        for q in range(self.peers):
            scale = table[:, self.peers + q:self.peers + q + 1] if self.gated else 1.0
            weights.append(jnp.where(table[:, q:q + 1] == lane, scale, 0.0).astype(BF16))
        vals = landed[k].reshape(self.peers * self.slots, self.half)
        sums[k] = jnp.dot(jnp.concatenate(weights, axis=1), vals, preferred_element_type=F32)

    def sum_and_send(self):
        _, y, x, core = self.spot
        side = self.side
        for copy in self.own:
            copy.wait()
        arrive(self.first)
        sel_l = self.selector([y * self.peers + q for q in range(self.peers)])
        sel_r = self.selector([((q // CORES) * side + x) * CORES + q % CORES for q in range(self.peers)])
        def both(i, carry):
            ky, kx = (y + i) % side, (x + i) % side
            self.partial(self.meta[ky, x, core], sel_l, self.r1l, self.ps_l, ky)
            self.partial(self.meta[y, kx, core], sel_r, self.r1r, self.ps_r, kx)
            return carry

        lax.fori_loop(1, side + 1, both, 0)
        start(self.second_l + self.second_r)

    def total(self, base, out_ref):
        _, y, x, core = self.spot
        half = self.half
        arrive(self.second_l + self.second_r)
        for cols, sums, k, landed in ((slice(0, half), self.ps_l, y, self.p2l), (slice(half, 2 * half), self.ps_r, x, self.p2r)):
            total = sums[k] if base is None else base[:, cols].astype(F32) + sums[k]
            for i in range(1, self.side):
                total = total + landed[i - 1]
            out_ref[:, cols] = total.astype(BF16)

    def drain(self):
        sent(self.first + self.second_l + self.second_r)


def return_moves(side):
    return [(k, dc) for k in range(1, side) for dc in range(CORES)] + [(0, 1)]


RETURN_BUFFERS = 6


def return_kernel(side, experts, head_dim, slots_b, u_all, meta_ref, w1_ref, w2_ref, w3_ref, h_ref, x_ref, dy_ref, gains_ref, wq, wk, wv, wo, y_ref, dx_ref, gq, gk, gv, go, gn, fwd_ref, meta, w13, w2, utile, recv, otile, du_s, *rest):
    bufs_b, bufs_a, rest = rest[:RETURN_BUFFERS], rest[RETURN_BUFFERS:2 * RETURN_BUFFERS], rest[2 * RETURN_BUFFERS:]
    att, rest = rest[:11], rest[11:]
    sems_b, sems_a, (loc, tin, tout) = rest[:5], rest[5:10], rest[10:]
    me, y, x, core = place_of(side)
    partners = [(y, (x + k) % side, (core + dc) % CORES) for k, dc in return_moves(side)]
    partners += [((y + k) % side, x, (core + dc) % CORES) for k, dc in return_moves(side) if k]
    greet([dev(side, *spot) for spot in partners])
    back_b = Return(side, experts, 2 * experts, False, slots_b, meta, bufs_b, sems_b)
    back_a = Return(side, experts, 0, True, fwd_ref, meta, bufs_a, sems_a)
    back_b.launch()
    width = w2_ref.shape[0]
    slots = fwd_ref.shape[3]
    dim = x_ref.shape[-1]
    loads = [pltpu.make_async_copy(meta_ref, meta, loc.at[0]), pltpu.make_async_copy(w2_ref, w2, loc.at[1]),
             pltpu.make_async_copy(w1_ref, w13.at[:, pl.ds(0, width)], loc.at[2]), pltpu.make_async_copy(w3_ref, w13.at[:, pl.ds(width, width)], loc.at[3])]
    start(loads)
    steps = side * side
    spot = lax.broadcasted_iota(jnp.int32, (slots, 1), 0).astype(F32) + 1.0

    def fetch(g, slot):
        return pltpu.make_async_copy(u_all.at[g // side, g % side], utile.at[slot], tin.at[slot])

    def put(g, slot):
        return pltpu.make_async_copy(otile.at[slot], fwd_ref.at[g // side, g % side], tout.at[slot])

    fetch(0, 0).start()
    for copy in loads:
        copy.wait()

    def step(g, carry):
        slot = g % 2
        fetch(g, slot).wait()

        @pl.when(g + 1 < steps)
        def _():
            fetch(g + 1, 1 - slot).start()
        for j in range(CORES):
            lines = my_rows(meta[g // side, g % side, j], experts, me, 0)
            pick = jnp.where(lines[0:1] == spot, 1.0, 0.0).astype(BF16)
            recv[pl.ds(j * slots, slots), :] = jnp.dot(pick, utile[slot, j], preferred_element_type=F32).astype(BF16)
        act = jnp.dot(recv[...], w13[...], preferred_element_type=F32).astype(BF16).astype(F32)
        act_1, act_3 = act[:, :width], act[:, width:]
        hidden = (act_1 * jax.nn.sigmoid(act_1) * act_3).astype(BF16)

        @pl.when(g >= 2)
        def _():
            put(g - 2, slot).wait()
        otile[slot] = jnp.dot(hidden, w2[...], preferred_element_type=F32).astype(BF16).reshape(CORES, slots, dim)
        put(g, slot).start()
        return carry

    lax.fori_loop(0, steps, step, 0)
    put(steps - 2, steps % 2).wait()
    put(steps - 1, 1 - steps % 2).wait()
    back_a.launch()
    q_s, k_s, v_s, ctx_s, normed_s = att[:5]
    attn = attention_rows(x_ref, gains_ref[0:1].astype(F32), wq, wk, wv, wo, head_dim, q_s, k_s, v_s, ctx_s, normed_s)
    att[10][...] = (x_ref[...].astype(F32) + attn.astype(BF16).astype(F32)).astype(BF16)
    back_b.sum_and_send()
    back_a.sum_and_send()
    back_b.total(None, du_s)
    attention_backward(head_dim, x_ref, dy_ref, du_s, gains_ref, wq, wk, wv, wo, dx_ref, gq, gk, gv, go, gn, *att)
    back_a.total(h_ref, y_ref)
    back_b.drain()
    back_a.drain()


def run_returns(slots_b, u_all, meta, experts_w, h_a, x_b, dy_b, gains, flat, head_dim, group):
    side = meta.shape[0]
    capacity, dim = slots_b.shape[1:]
    rows = x_b.shape[0]
    half = dim // 2
    peers = side * CORES
    width = experts_w[1].shape[0]
    full, kv = flat[0].shape[1], flat[1].shape[1]
    any_spec, vmem = pl.BlockSpec(memory_space=pl.ANY), pl.BlockSpec(memory_space=pltpu.VMEM)
    cube = slots_b.reshape(side, side, CORES, capacity, dim)
    sets = [pltpu.VMEM((side, peers, capacity, half), BF16)] * 2 + [pltpu.VMEM((side, rows, half), F32)] * 2 + [pltpu.VMEM((side - 1, rows, half), F32)] * 2
    sems = [pltpu.SemaphoreType.DMA((2,)), pltpu.SemaphoreType.DMA((2, peers)), pltpu.SemaphoreType.DMA((2, peers)), pltpu.SemaphoreType.DMA((2, side)), pltpu.SemaphoreType.DMA((2, side))]
    return pl.pallas_call(
        functools.partial(return_kernel, side, group, head_dim),
        out_shape=[jax.ShapeDtypeStruct(x_b.shape, BF16)] * 2 + [jax.ShapeDtypeStruct(part.shape, BF16) for part in flat] + [jax.ShapeDtypeStruct((2, dim), F32), jax.ShapeDtypeStruct(cube.shape, BF16)],
        in_specs=[any_spec] * 6 + [vmem] * 8,
        out_specs=[vmem] * 7 + [any_spec],
        scratch_shapes=[
            pltpu.VMEM(meta.shape, BF16),
            pltpu.VMEM((dim, 2 * width), BF16),
            pltpu.VMEM((width, dim), BF16),
            pltpu.VMEM((2, CORES, rows, dim), BF16),
            pltpu.VMEM((CORES * capacity, dim), BF16),
            pltpu.VMEM((2, CORES, capacity, dim), BF16),
            pltpu.VMEM((rows, dim), BF16),
        ] + sets + sets + [pltpu.VMEM((rows, cols), BF16) for cols in (full, kv, kv, full, dim, full, full, kv, kv, dim, dim)] + sems + sems + [pltpu.SemaphoreType.DMA((4,)), pltpu.SemaphoreType.DMA((2,)), pltpu.SemaphoreType.DMA((2,))],
        compiler_params=pltpu.CompilerParams(collective_id=1, has_side_effects=True, vmem_limit_bytes=67043328),
    )(cube, u_all, meta, *experts_w, h_a, x_b, dy_b, gains, *flat)


def solution(mesh):
    group = mesh.shape['expert']

    def local_step(x_a, x_b, dy_b, eid_a, slot_a, gate_a, eid_b, slot_b, gate_b, u_b, norm_1, norm_2, w_q, w_k, w_v, w_o, w_1, w_2, w_3):
        rows, model_dim = x_a.shape
        w1, w2, w3 = w_1[0], w_2[0], w_3[0]

        head_dim = w_q.shape[2]
        gains = jnp.stack([norm_1, norm_2])
        routes = tuple(part.T for part in (eid_a, slot_a, gate_a, eid_b, slot_b, gate_b))
        flat = (w_q.reshape(model_dim, -1), w_k.reshape(model_dim, -1), w_v.reshape(model_dim, -1), w_o.reshape(-1, model_dim))

        u_all, meta, grad_in, grad_w1, grad_w2, grad_w3, h_a = run_backward(dy_b, x_a, routes, u_b[0], (w1, w2, w3, gains) + flat, head_dim, group)
        y_a, dx_b, g_q, g_k, g_v, g_o, g_n, _ = run_returns(grad_in, u_all, meta, (w1, w2, w3), h_a, x_b, dy_b, gains, flat, head_dim, group)
        grads = tuple(g.reshape(w.shape).astype(F32)[None] for g, w in ((g_q, w_q), (g_k, w_k), (g_v, w_v), (g_o, w_o))) + (g_n[0:1], g_n[1:2])
        return (y_a, dx_b, grad_w1[None], grad_w2[None], grad_w3[None], *grads)

    row_spec = P(('data', 'expert'), None)
    cube_spec = P(('data', 'expert'), None, None)
    quad_spec = P(('data', 'expert'), None, None, None)
    expert_spec = P('expert', None, None)
    in_specs = (row_spec, row_spec, row_spec, row_spec, row_spec, row_spec, row_spec, row_spec, row_spec, cube_spec, P(), P(), P(), P(), P(), P(), expert_spec, expert_spec, expert_spec)
    out_specs = (row_spec, row_spec, cube_spec, cube_spec, cube_spec, quad_spec, quad_spec, quad_spec, quad_spec, row_spec, row_spec)
    return jax.shard_map(local_step, mesh=mesh, in_specs=in_specs, out_specs=out_specs, check_vma=False)
```
